32 devices in a mesh: dev: 32 (over z, y, x, core).
Axes of the slice: x: 2, y: 2, z: 4, core: 2. Of those that a mesh axis runs over, the one named last changes fastest.
Arguments:
- tokens: bfloat16 [24576, 768], P('dev'), may hold values from -6 to 6
- cotangent: bfloat16 [24576, 768], P('dev'), may hold values from -6 to 6
- clip_start: int32 [24576], P('dev'), may hold values from 0 to 24575, as said below
- clip_end: int32 [24576], P('dev'), may hold values from 1 to 24576, as said below
- qkv_weight: float32 [3, 768, 768], P(None, 'dev'), may hold values from -0.21875 to 0.21875
- out_weight: float32 [768, 768], P('dev'), may hold values from -4 to 4
- up_weight: float32 [768, 3072], P('dev'), may hold values from -0.21875 to 0.21875
- down_weight: float32 [3072, 768], P('dev'), may hold values from -0.109375 to 0.109375
- vectors: float32 [12, 768], P(None, 'dev'), may hold values from -1.6 to 1.6, as said below
- qkv_first: float32 [3, 768, 768], P(None, 'dev'), may hold values from -48 to 48
- out_first: float32 [768, 768], P('dev'), may hold values from -48 to 48
- up_first: float32 [768, 3072], P('dev'), may hold values from -48 to 48
- down_first: float32 [3072, 768], P('dev'), may hold values from -48 to 48
- vector_first: float32 [12, 768], P(None, 'dev'), may hold values from -48 to 48
- qkv_second: float32 [3, 768, 768], P(None, 'dev'), may hold values from 7.3728 to 73.728
- out_second: float32 [768, 768], P('dev'), may hold values from 7.3728 to 73.728
- up_second: float32 [768, 3072], P('dev'), may hold values from 7.3728 to 73.728
- down_second: float32 [3072, 768], P('dev'), may hold values from 7.3728 to 73.728
- vector_second: float32 [12, 768], P(None, 'dev'), may hold values from 7.3728 to 73.728
Outputs:
- result: bfloat16 [24576, 768], P('dev')
- grad_tokens: float32 [24576, 768], P('dev')
- qkv_update: float32 [3, 768, 768], P(None, 'dev')
- out_update: float32 [768, 768], P('dev')
- up_update: float32 [768, 3072], P('dev')
- down_update: float32 [3072, 768], P('dev')
- vector_update: float32 [12, 768], P(None, 'dev')
- qkv_first_new: float32 [3, 768, 768], P(None, 'dev')
- out_first_new: float32 [768, 768], P('dev')
- up_first_new: float32 [768, 3072], P('dev')
- down_first_new: float32 [3072, 768], P('dev')
- vector_first_new: float32 [12, 768], P(None, 'dev')
- qkv_second_new: float32 [3, 768, 768], P(None, 'dev')
- out_second_new: float32 [768, 768], P('dev')
- up_second_new: float32 [768, 3072], P('dev')
- down_second_new: float32 [3072, 768], P('dev')
- vector_second_new: float32 [12, 768], P(None, 'dev')
The draws below stay inside these ranges and needn't reach their ends.
Inputs may be any that keep to these rules, and one draw needn't show every extreme that they name: clip_start[i] <= i < clip_start[i] + 1500; clips lie end to end and all tokens of a clip share clip_start; the first clip starts at 0 and holds 1500 tokens. clip_start[i] < clip_end[i] <= clip_start[i] + 1500, equal to it for the first clip; all tokens of a clip share clip_end; tokens of a clip at or after clip_end are padding. `vectors`: rows 0 and 5 lie near 1.
All inputs are finite; a program needn't handle non-finite values.
Results may differ from the reference program's by a relative error of at most 0.023.
Values may be sent and summed in bfloat16 or wider, within the bound.
A program may use at most 384 MiB of HBM per device.

```python
import math
import jax
import jax.numpy as jnp
from jax import lax

D = 768
H = 12
HD = 64
FF = 3072
TOK_DEV = 768
CLIP = 1500
STEP = 10
TOKENS = 24576
N_DEV = 32


def clip_bounds(key):
    base_key = jax.random.fold_in(key, 7)
    clip_count = TOKENS // (CLIP // 2) + 2
    spans = jax.random.randint(jax.random.fold_in(base_key, 1), (clip_count,), CLIP // 2, CLIP + 1).astype(jnp.int32)
    spans = spans.at[0].set(CLIP)
    ends = jnp.cumsum(spans).astype(jnp.int32)
    starts = ends - spans
    cuts = jax.random.randint(jax.random.fold_in(base_key, 2), (clip_count,), 0, 1 << 20).astype(jnp.int32)
    audio = spans - cuts % (spans // 2 + 1)
    audio = audio.at[0].set(CLIP)
    positions = jnp.arange(TOKENS, dtype=jnp.int32)
    which_clip = jnp.sum((ends[None, :] <= positions[:, None]).astype(jnp.int32), axis=1)
    one_hot = (jnp.arange(clip_count, dtype=jnp.int32)[None, :] == which_clip[:, None]).astype(jnp.int32)
    begin = jnp.sum(one_hot * starts[None, :], axis=1)
    finish = jnp.minimum(jnp.sum(one_hot * (starts + audio)[None, :], axis=1), TOKENS)
    return (begin.astype(jnp.int32), finish.astype(jnp.int32))


def draw_clip_start(key, part):
    return clip_bounds(key)[0]


def draw_clip_end(key, part):
    return clip_bounds(key)[1]


def draw_vectors(key, part):
    spread = jnp.clip(jax.random.normal(jax.random.fold_in(key, 4), (12, D), jnp.float32), -3.5, 3.5)
    row_index = jnp.arange(12)[:, None]
    is_gain = (row_index == 0) | (row_index == 5)
    return jnp.where(is_gain, 1.0 + 0.15 * spread, 0.45 * spread).astype(jnp.float32)


def block_scale(own_key, shape, pieces, smallest, top_value):
    def one(dim, parts):
        draws = jax.random.uniform(jax.random.fold_in(jax.random.fold_in(own_key, 6), dim), (parts,), jnp.float32, smallest / len(pieces), top_value / len(pieces))
        return jnp.repeat(jnp.exp(draws), shape[dim] // parts).reshape((-1,) + (1,) * (len(shape) - dim - 1))

    factor_of = one(*pieces[0])
    for cut in pieces[1:]:
        factor_of = factor_of * one(*cut)
    return factor_of


def centred(key, dims, scale, limit, shards=(), held_as=jnp.bfloat16):
    result = jax.random.normal(key, dims, jnp.float32) * scale
    if len(shards) > 0:
        result = block_scale(key, dims, shards, -0.22, 0.18) * result
    return jnp.clip(result, min=-limit, max=limit).astype(held_as)


def setup_inputs(seed: int = 0) -> dict:
    splits = jax.random.split(jax.random.key(seed), 20)
    return {
        "tokens": centred(splits[0], (TOKENS, D), 1.0, 6.0, ((0, 32),)),
        "cotangent": centred(splits[1], (TOKENS, D), 1.0, 6.0, ((0, 32),)),
        "clip_start": draw_clip_start(jax.random.fold_in(splits[19], 71), 0),
        "clip_end": draw_clip_end(jax.random.fold_in(splits[19], 71), 0),
        "qkv_weight": centred(splits[4], (3, D, D), D ** -0.5, 0.21875, ((1, 32),), jnp.float32),
        "out_weight": centred(splits[5], (D, D), (max(2, 3 * D // CLIP)) ** -0.5, 4.0, ((0, 32),), jnp.float32),
        "up_weight": centred(splits[6], (D, FF), D ** -0.5, 0.21875, ((0, 32),), jnp.float32),
        "down_weight": centred(splits[7], (FF, D), FF ** -0.5, 0.109375, ((0, 32),), jnp.float32),
        "vectors": draw_vectors(jax.random.fold_in(splits[19], 71), 0),
        "qkv_first": centred(splits[9], (3, D, D), (0.05 * TOKENS ** 0.5), 48.0, ((1, 32),), jnp.float32),
        "out_first": centred(splits[10], (D, D), (0.05 * TOKENS ** 0.5), 48.0, ((0, 32),), jnp.float32),
        "up_first": centred(splits[11], (D, FF), (0.05 * TOKENS ** 0.5), 48.0, ((0, 32),), jnp.float32),
        "down_first": centred(splits[12], (FF, D), (0.05 * TOKENS ** 0.5), 48.0, ((0, 32),), jnp.float32),
        "vector_first": centred(splits[13], (12, D), (0.05 * TOKENS ** 0.5), 48.0, ((1, 32),), jnp.float32),
        "qkv_second": jnp.clip(jnp.exp(math.log(73.728) - 2.3025851 * jax.random.uniform(splits[14], (3, D, D), jnp.float32) ** block_scale(splits[14], (3, D, D), ((1, 32),), -0.2, 0.2)), 7.3728, 73.728),
        "out_second": jnp.clip(jnp.exp(math.log(73.728) - 2.3025851 * jax.random.uniform(splits[15], (D, D), jnp.float32) ** block_scale(splits[15], (D, D), ((0, 32),), -0.2, 0.2)), 7.3728, 73.728),
        "up_second": jnp.clip(jnp.exp(math.log(73.728) - 2.3025851 * jax.random.uniform(splits[16], (D, FF), jnp.float32) ** block_scale(splits[16], (D, FF), ((0, 32),), -0.2, 0.2)), 7.3728, 73.728),
        "down_second": jnp.clip(jnp.exp(math.log(73.728) - 2.3025851 * jax.random.uniform(splits[17], (FF, D), jnp.float32) ** block_scale(splits[17], (FF, D), ((0, 32),), -0.2, 0.2)), 7.3728, 73.728),
        "vector_second": jnp.clip(jnp.exp(math.log(73.728) - 2.3025851 * jax.random.uniform(splits[18], (12, D), jnp.float32) ** block_scale(splits[18], (12, D), ((1, 32),), -0.2, 0.2)), 7.3728, 73.728),
    }


@jax.custom_vjp
def low(v):
    return lax.optimization_barrier(v.astype(jnp.bfloat16)).astype(jnp.float32)

@jax.custom_vjp
def low_back(v):
    return v

def low_keep(v):
    return (low(v), None)

def low_pass(kept, grad):
    return (grad,)

def back_keep(v):
    return (v, None)

def back_low(kept, grad):
    return (low(grad),)
low.defvjp(low_keep, low_pass)
low_back.defvjp(back_keep, back_low)
precise = lax.Precision.HIGHEST
masked_score = -1e+30

def layer_norm(values, gain_row, bias_row):
    centre = values - lax.optimization_barrier(jnp.mean(values, axis=-1, keepdims=True))
    spread = lax.optimization_barrier(jnp.mean(centre * centre, axis=-1, keepdims=True))
    return centre * lax.rsqrt(spread + 1e-05) * gain_row + bias_row

def exact_gelu(values):
    return jax.nn.gelu(values, approximate=False)

def clip_attention(query, keys, values, clip_start, clip_end):
    window = TOK_DEV + 2 * CLIP
    score_scale = HD ** (-0.5)

    def one_block(block_first):
        query_rows = lax.dynamic_slice_in_dim(query, block_first, TOK_DEV, 0).reshape(TOK_DEV, H, HD)
        key_first = jnp.clip(block_first - CLIP, 0, TOKENS - window).astype(jnp.int32)
        key_rows = lax.dynamic_slice_in_dim(keys, key_first, window, 0).reshape(window, H, HD)
        value_rows = lax.dynamic_slice_in_dim(values, key_first, window, 0).reshape(window, H, HD)
        lower_bound = lax.dynamic_slice_in_dim(clip_start, block_first, TOK_DEV, 0)
        upper_bound = lax.dynamic_slice_in_dim(clip_end, block_first, TOK_DEV, 0)
        places = key_first + jnp.arange(window, dtype=jnp.int32)
        allowed = (places[None, :] >= lower_bound[:, None]) & (places[None, :] < upper_bound[:, None])
        scores = low_back(jnp.einsum('qhd,khd->hqk', query_rows, key_rows, precision=precise) * score_scale)
        scores = jnp.where(allowed[None], scores, masked_score)
        peak = lax.optimization_barrier(jnp.max(scores, axis=-1, keepdims=True))
        weights = jnp.exp(scores - peak)
        weights = low(weights / lax.optimization_barrier(jnp.sum(weights, axis=-1, keepdims=True)))
        mixed = jnp.einsum('hqk,khd->qhd', weights, value_rows, precision=precise)
        return mixed.reshape(TOK_DEV, H * HD)
    block_starts = jnp.arange(N_DEV, dtype=jnp.int32) * TOK_DEV
    mixed = lax.map(jax.checkpoint(one_block), block_starts).reshape(TOKENS, H * HD)
    return low_back(low(mixed))

def layer_forward(tokens_wide, qkv_copy, out_copy, up_copy, down_copy, vector_copy, clip_start, clip_end):
    normed = low(layer_norm(tokens_wide, vector_copy[0], vector_copy[1]))
    query = low_back(low(jnp.dot(normed, qkv_copy[0], precision=precise) + vector_copy[2]))
    keys = low_back(low(jnp.dot(normed, qkv_copy[1], precision=precise)))
    values = low_back(low(jnp.dot(normed, qkv_copy[2], precision=precise) + vector_copy[3]))
    mixed = clip_attention(query, keys, values, clip_start, clip_end)
    branch = low_back(jnp.dot(mixed, out_copy, precision=precise) + vector_copy[4])
    middle = tokens_wide + branch
    normed_two = low(layer_norm(middle, vector_copy[5], vector_copy[6]))
    up_bias = vector_copy[8:12].reshape(FF)
    hidden = low_back(jnp.dot(normed_two, up_copy, precision=precise) + up_bias)
    active = low(exact_gelu(hidden))
    return middle + jnp.dot(active, down_copy, precision=precise) + vector_copy[7]

def adamw_step(master, gradient, first_moment, second_moment):
    first_new = 0.9 * first_moment + 0.1 * gradient
    second_new = 0.999 * second_moment + 0.001 * gradient * gradient
    fix_one = 1.0 - 0.9 ** STEP
    fix_two = 1.0 - 0.999 ** STEP
    update = -0.02 * (first_new / fix_one / (jnp.sqrt(second_new / fix_two) + 1e-08) + 0.1 * master)
    return (update, first_new, second_new)

def reference(tokens, cotangent, clip_start, clip_end, qkv_weight, out_weight, up_weight, down_weight, vectors, qkv_first, out_first, up_first, down_first, vector_first, qkv_second, out_second, up_second, down_second, vector_second):
    masters = (qkv_weight, out_weight, up_weight, down_weight, vectors)
    copies = tuple((master.astype(jnp.bfloat16).astype(jnp.float32) for master in masters))

    def forward(tokens_wide, qkv_copy, out_copy, up_copy, down_copy, vector_copy):
        return layer_forward(tokens_wide, qkv_copy, out_copy, up_copy, down_copy, vector_copy, clip_start, clip_end)
    output_wide, pullback = jax.vjp(forward, tokens.astype(jnp.float32), copies[0], copies[1], copies[2], copies[3], copies[4])
    gradients = pullback(cotangent.astype(jnp.float32))
    firsts = (qkv_first, out_first, up_first, down_first, vector_first)
    seconds = (qkv_second, out_second, up_second, down_second, vector_second)
    stepped = [adamw_step(masters[place], gradients[place + 1], firsts[place], seconds[place]) for place in range(5)]
    return (output_wide.astype(jnp.bfloat16), gradients[0], stepped[0][0], stepped[1][0], stepped[2][0], stepped[3][0], stepped[4][0], stepped[0][1], stepped[1][1], stepped[2][1], stepped[3][1], stepped[4][1], stepped[0][2], stepped[1][2], stepped[2][2], stepped[3][2], stepped[4][2])
```

```python
import functools

import jax
import jax.numpy as jnp
from jax import lax
from jax.experimental import pallas as pl
from jax.experimental.pallas import tpu as pltpu
from jax.sharding import PartitionSpec as P

HD = 64
CLIP = 1500
STEP = 10
LANE = 128
FAR = 1 << 30
SQRT_HALF = 0.7071067811865476
INV_SQRT_TWO_PI = 0.3989422804014327


beta_one = 0.9
beta_two = 0.999
learn_rate = 0.02
weight_decay = 0.1
adam_eps = 1e-08
norm_eps = 1e-05
masked_score = -1e30
FORWARD_TILES = (256, 384)
QUERY_TILES = (256, 256)
KEY_TILES = (256, 256)
PROJECT_TILE = 768
MIDDLE_TILE = 256
MIDDLE_CHUNK = 512
LAST_TILE = 256
GROUP = 2
NT = (((1,), (1,)), ((), ()))
NN = (((1,), (0,)), ((), ()))


def shifted(value, axis, steps):
    count = lax.axis_size(axis)
    initial, last = (max(0, -steps), min(count, count - steps))
    return lax.ppermute(value, axis, [(source, source + steps) for source in range(initial, last)])


def dot(a, b, dims=NN):
    return lax.dot_general(a, b, dims, preferred_element_type=jnp.float32)


def stacked(pair, scale):
    lane = lax.broadcasted_iota(jnp.int32, pair.shape, 1)
    zero = jnp.zeros_like(pair)
    if scale is not None:
        pair = pair * jnp.asarray(scale, pair.dtype)
    return jnp.concatenate([jnp.where(lane < HD, pair, zero), jnp.where(lane >= HD, pair, zero)], axis=0)


def unstacked(both):
    rows = both.shape[0] // 2
    lane = lax.broadcasted_iota(jnp.int32, (rows, LANE), 1)
    return jnp.where(lane < HD, both[:rows], both[rows:])


def column(table, place):
    lane = lax.broadcasted_iota(jnp.int32, table.shape, 1)
    return jnp.sum(jnp.where(lane == place, table, 0.0), axis=1, keepdims=True)


def forward_kernel(tq, tk, pairs, bounds, lower, upper, q_ref, k_ref, v_ref, o_ref, lse_ref, qs, peak, acc):
    group = pl.program_id(0)
    tiles = q_ref.shape[0] // tq
    ones = jnp.ones((tk, LANE), jnp.bfloat16)

    @pl.when(group == 0)
    def _():
        lse_ref[...] = jnp.zeros_like(lse_ref)

    def one_tile(tile, none):
        rows = pl.ds(pl.multiple_of(tile * tq, tq), tq)
        for pair in range(pairs):
            qs[pair] = stacked(q_ref[rows, pair * LANE : (pair + 1) * LANE], HD ** -0.5)
        peak[...] = jnp.full_like(peak, masked_score)
        acc[...] = jnp.zeros_like(acc)
        low, high = lower[rows, :], upper[rows, :]

        def step(key_tile, none):
            first = pl.multiple_of(key_tile * tk, tk)
            places = first + lax.broadcasted_iota(jnp.int32, (tq, tk), 1)
            bias = jnp.where((places >= low) & (places < high), 0.0, masked_score)
            bias = jnp.concatenate([bias, bias], axis=0)
            for pair in range(pairs):
                lanes = slice(pair * LANE, (pair + 1) * LANE)
                scores = dot(qs[pair], k_ref[pl.ds(first, tk), lanes], NT) + bias
                old = peak[pair]
                new = jnp.maximum(old, jnp.max(scores, axis=1, keepdims=True))
                peak[pair] = new
                weights = jnp.exp(scores - new[:, :1]).astype(jnp.bfloat16)
                values = jnp.concatenate([v_ref[pl.ds(first, tk), lanes], ones], axis=1)
                scale = jnp.exp(old - new)
                acc[pair] = acc[pair] * jnp.concatenate([scale, scale], axis=1) + dot(weights, values)
            return none

        lax.fori_loop(bounds[2 * tile], bounds[2 * tile + 1], step, 0)
        lane = lax.broadcasted_iota(jnp.int32, (tq, LANE), 1)
        table = lse_ref[rows, :]
        for pair in range(pairs):
            both = acc[pair]
            total = both[:, LANE:]
            o_ref[rows, pair * LANE : (pair + 1) * LANE] = unstacked(both[:, :LANE] / total).astype(o_ref.dtype)
            logs = peak[pair] + jnp.log(total)
            head = (group * pairs + pair) * 2
            table = jnp.where(lane == head, logs[:tq], table)
            table = jnp.where(lane == head + 1, logs[tq:], table)
        lse_ref[rows, :] = table
        return none

    lax.fori_loop(0, tiles, one_tile, 0)


def attend(query, keys, values, lower, upper, bounds, tq, tk, pairs):
    rows, width = query.shape
    window = keys.shape[0]
    lanes = pairs * LANE
    return pl.pallas_call(
        functools.partial(forward_kernel, tq, tk, pairs),
        grid_spec=pltpu.PrefetchScalarGridSpec(
            num_scalar_prefetch=1, grid=(width // lanes,),
            in_specs=[
                pl.BlockSpec((rows, 1), lambda g, b: (0, 0)),
                pl.BlockSpec((rows, 1), lambda g, b: (0, 0)),
                pl.BlockSpec((rows, lanes), lambda g, b: (0, g)),
                pl.BlockSpec((window, lanes), lambda g, b: (0, g)),
                pl.BlockSpec((window, lanes), lambda g, b: (0, g)),
            ],
            out_specs=[pl.BlockSpec((rows, lanes), lambda g, b: (0, g)), pl.BlockSpec((rows, LANE), lambda g, b: (0, 0))],
            scratch_shapes=[
                pltpu.VMEM((pairs, 2 * tq, LANE), jnp.bfloat16),
                pltpu.VMEM((pairs, 2 * tq, LANE), jnp.float32),
                pltpu.VMEM((pairs, 2 * tq, 2 * LANE), jnp.float32),
            ],
        ),
        out_shape=[jax.ShapeDtypeStruct((rows, width), jnp.bfloat16), jax.ShapeDtypeStruct((rows, LANE), jnp.float32)],
        name="attend",
    )(bounds, lower, upper, query, keys, values)


def query_grad_kernel(tq, tk, pairs, bounds, lower, upper, q_ref, g_ref, k_ref, v_ref, lse_ref, delta_ref, dq_ref, qs, gs, logs, deltas, acc):
    group = pl.program_id(0)
    tiles = q_ref.shape[0] // tq

    def one_tile(tile, none):
        rows = pl.ds(pl.multiple_of(tile * tq, tq), tq)
        table, other = lse_ref[rows, :], delta_ref[rows, :]
        for pair in range(pairs):
            lanes = slice(pair * LANE, (pair + 1) * LANE)
            qs[pair] = stacked(q_ref[rows, lanes], HD ** -0.5)
            gs[pair] = stacked(g_ref[rows, lanes], None)
            head = (group * pairs + pair) * 2
            logs[pair] = jnp.broadcast_to(jnp.concatenate([column(table, head), column(table, head + 1)], axis=0), logs.shape[1:])
            deltas[pair] = jnp.broadcast_to(jnp.concatenate([column(other, head), column(other, head + 1)], axis=0), logs.shape[1:])
        acc[...] = jnp.zeros_like(acc)
        low, high = lower[rows, :], upper[rows, :]

        def step(key_tile, none):
            first = pl.multiple_of(key_tile * tk, tk)
            places = first + lax.broadcasted_iota(jnp.int32, (tq, tk), 1)
            bias = jnp.where((places >= low) & (places < high), 0.0, masked_score)
            bias = jnp.concatenate([bias, bias], axis=0)
            for pair in range(pairs):
                lanes = slice(pair * LANE, (pair + 1) * LANE)
                keys = k_ref[pl.ds(first, tk), lanes]
                scores = dot(qs[pair], keys, NT) + bias
                probs = jnp.exp(scores - logs[pair][:, :1])
                grad_probs = dot(gs[pair], v_ref[pl.ds(first, tk), lanes], NT)
                grad_scores = (probs * (grad_probs - deltas[pair][:, :1])).astype(jnp.bfloat16)
                acc[pair] += dot(grad_scores, keys)
            return none

        lax.fori_loop(bounds[2 * tile], bounds[2 * tile + 1], step, 0)
        for pair in range(pairs):
            dq_ref[rows, pair * LANE : (pair + 1) * LANE] = (unstacked(acc[pair]) * HD ** -0.5).astype(dq_ref.dtype)
        return none

    lax.fori_loop(0, tiles, one_tile, 0)


def query_grad(query, grad, keys, values, lse, delta, lower, upper, bounds, tq, tk, pairs):
    rows, width = query.shape
    window = keys.shape[0]
    lanes = pairs * LANE
    own = lambda: pl.BlockSpec((rows, lanes), lambda g, b: (0, g))
    far = lambda: pl.BlockSpec((window, lanes), lambda g, b: (0, g))
    fixed = lambda cols: pl.BlockSpec((rows, cols), lambda g, b: (0, 0))
    return pl.pallas_call(
        functools.partial(query_grad_kernel, tq, tk, pairs),
        grid_spec=pltpu.PrefetchScalarGridSpec(
            num_scalar_prefetch=1, grid=(width // lanes,),
            in_specs=[fixed(1), fixed(1), own(), own(), far(), far(), fixed(LANE), fixed(LANE)],
            out_specs=own(),
            scratch_shapes=[
                pltpu.VMEM((pairs, 2 * tq, LANE), jnp.bfloat16),
                pltpu.VMEM((pairs, 2 * tq, LANE), jnp.bfloat16),
                pltpu.VMEM((pairs, 2 * tq, LANE), jnp.float32),
                pltpu.VMEM((pairs, 2 * tq, LANE), jnp.float32),
                pltpu.VMEM((pairs, 2 * tq, LANE), jnp.float32),
            ],
        ),
        out_shape=jax.ShapeDtypeStruct((rows, width), jnp.bfloat16),
        name="query_grad",
    )(bounds, lower, upper, query, grad, keys, values, lse, delta)


def key_grad_kernel(tk, tq, pairs, base, bounds, lower, upper, k_ref, v_ref, q_ref, g_ref, lse_ref, delta_ref, dk_ref, dv_ref, ks, vs, acc):
    tiles = k_ref.shape[0] // tk

    def one_tile(tile, none):
        rows = pl.ds(pl.multiple_of(tile * tk, tk), tk)
        for pair in range(pairs):
            lanes = slice(pair * LANE, (pair + 1) * LANE)
            ks[pair] = stacked(k_ref[rows, lanes], HD ** -0.5)
            vs[pair] = stacked(v_ref[rows, lanes], None)
        acc[...] = jnp.zeros_like(acc)

        def step(query_tile, none):
            first = pl.multiple_of(query_tile * tq, tq)
            here = pl.ds(first, tq)
            places = base + tile * tk + lax.broadcasted_iota(jnp.int32, (tk, tq), 0)
            bias = jnp.where((places >= lower[:, here]) & (places < upper[:, here]), 0.0, masked_score)
            for pair in range(pairs):
                lanes = slice(pair * LANE, (pair + 1) * LANE)
                queries, grads = q_ref[here, lanes], g_ref[here, lanes]
                scores = dot(ks[pair], queries, NT)
                grad_probs = dot(vs[pair], grads, NT)
                probs, grad_scores = [], []
                for half in range(2):
                    part = slice(half * tk, (half + 1) * tk)
                    head = slice(2 * pair + half, 2 * pair + half + 1)
                    prob = jnp.exp(scores[part] + bias - lse_ref[0, head, here])
                    probs.append(prob.astype(jnp.bfloat16))
                    grad_scores.append((prob * (grad_probs[part] - delta_ref[0, head, here])).astype(jnp.bfloat16))
                acc[pair, :, :LANE] += dot(jnp.concatenate(grad_scores, axis=0), queries)
                acc[pair, :, LANE:] += dot(jnp.concatenate(probs, axis=0), grads)
            return none

        lax.fori_loop(bounds[2 * tile], bounds[2 * tile + 1], step, 0)
        for pair in range(pairs):
            lanes = slice(pair * LANE, (pair + 1) * LANE)
            dk_ref[rows, lanes] = (unstacked(acc[pair, :, :LANE]) * HD ** -0.5).astype(dk_ref.dtype)
            dv_ref[rows, lanes] = unstacked(acc[pair, :, LANE:]).astype(dv_ref.dtype)
        return none

    lax.fori_loop(0, tiles, one_tile, 0)


def key_grad(keys, values, query, grad, lse, delta, lower, upper, bounds, base, tk, tq, pairs):
    rows, width = keys.shape
    window = query.shape[0]
    lanes = pairs * LANE
    own = lambda: pl.BlockSpec((rows, lanes), lambda g, b: (0, g))
    far = lambda: pl.BlockSpec((window, lanes), lambda g, b: (0, g))
    line = lambda: pl.BlockSpec((1, window), lambda g, b: (0, 0))
    heads = lambda: pl.BlockSpec((1, 2 * pairs, window), lambda g, b: (g, 0, 0))
    return pl.pallas_call(
        functools.partial(key_grad_kernel, tk, tq, pairs, base),
        grid_spec=pltpu.PrefetchScalarGridSpec(
            num_scalar_prefetch=1, grid=(width // lanes,),
            in_specs=[line(), line(), own(), own(), far(), far(), heads(), heads()],
            out_specs=[own(), own()],
            scratch_shapes=[
                pltpu.VMEM((pairs, 2 * tk, LANE), jnp.bfloat16),
                pltpu.VMEM((pairs, 2 * tk, LANE), jnp.bfloat16),
                pltpu.VMEM((pairs, 2 * tk, 2 * LANE), jnp.float32),
            ],
        ),
        out_shape=[jax.ShapeDtypeStruct((rows, width), jnp.bfloat16)] * 2,
        name="key_grad",
    )(bounds, lower, upper, keys, values, query, grad, lse, delta)


def units(values):
    centre = values - jnp.mean(values, axis=-1, keepdims=True)
    inverse = lax.rsqrt(jnp.mean(centre * centre, axis=-1, keepdims=True) + norm_eps)
    return centre * inverse, inverse


def norm_pull(grad_output, unit, inverse, gain):
    grad_unit = grad_output * gain
    first = jnp.mean(grad_unit, axis=-1, keepdims=True)
    second = jnp.mean(grad_unit * unit, axis=-1, keepdims=True)
    return inverse * (grad_unit - first - unit * second)


def row_sum(values):
    return jnp.sum(values, axis=0, keepdims=True)


def gelu_pair(hidden):
    inner = 0.5 + 0.5 * lax.erf(hidden * SQRT_HALF)
    slope = inner + hidden * (jnp.exp(-0.5 * hidden * hidden) * INV_SQRT_TWO_PI)
    return hidden * inner, slope


def project_kernel(tile, active, tokens, vectors, weights, query, keys, values):
    place = pl.program_id(0)
    needed = (place >= active[0]) & (place < active[1])

    @pl.when(needed)
    def _():
        unit = units(tokens[...].astype(jnp.float32))[0]
        normed = (unit * vectors[0:1, :] + vectors[1:2, :]).astype(jnp.bfloat16)
        query[...] = (dot(normed, weights[0]) + vectors[2:3, :]).astype(query.dtype)
        keys[...] = dot(normed, weights[1]).astype(keys.dtype)
        values[...] = (dot(normed, weights[2]) + vectors[3:4, :]).astype(values.dtype)

    @pl.when(jnp.logical_not(needed))
    def _():
        for out in (query, keys, values):
            out[...] = jnp.zeros_like(out)


def project(tokens, vectors, weights, active, tile):
    rows, width = tokens.shape
    block = lambda: pl.BlockSpec((tile, width), lambda i, b: (i, 0))
    return pl.pallas_call(
        functools.partial(project_kernel, tile),
        grid_spec=pltpu.PrefetchScalarGridSpec(
            num_scalar_prefetch=1, grid=(rows // tile,),
            in_specs=[
                block(),
                pl.BlockSpec(vectors.shape, lambda i, b: (0, 0)),
                pl.BlockSpec(weights.shape, lambda i, b: (0, 0, 0)),
            ],
            out_specs=[block(), block(), block()],
        ),
        out_shape=[jax.ShapeDtypeStruct((rows, width), jnp.bfloat16)] * 3,
        name="project",
    )(active, tokens, vectors, weights)


def middle_kernel(tile, tokens, mixed, cotangent, vectors, up_bias, out_weight, up_weight, down_weight,
                  result, grad_middle, grad_mixed, delta, grad_out, grad_up, grad_down, grad_rows, grad_bias,
                  middle, normed, turned, total, back, actives, hiddens):
    place, count = pl.program_id(0), pl.num_programs(0)
    rows = tokens.shape[0]
    parts = [slice(i, i + tile) for i in range(0, rows, tile)]

    @pl.when(place == 0)
    def _():
        for part in parts:
            branch = dot(mixed[part, :], out_weight[...]) + vectors[4:5, :]
            wide = tokens[part, :].astype(jnp.float32) + branch
            middle[part, :] = wide
            unit = units(wide)[0]
            low = (unit * vectors[5:6, :] + vectors[6:7, :]).astype(jnp.bfloat16)
            normed[part, :] = low
            turned[:, part] = low.T
            total[part, :] = wide + vectors[7:8, :]
        back[...] = jnp.zeros_like(back)

    bias = jnp.zeros_like(grad_bias)
    for part in parts:
        hidden = dot(normed[part, :], up_weight[...]) + up_bias[...]
        wide, slope = gelu_pair(hidden)
        active = wide.astype(jnp.bfloat16)
        grad_active = dot(cotangent[part, :], down_weight[...], NT)
        grad_hidden = (grad_active * slope).astype(jnp.bfloat16)
        actives[part, :] = active
        hiddens[part, :] = grad_hidden
        bias += row_sum(grad_hidden.astype(jnp.float32))
        total[part, :] += dot(active, down_weight[...])
        back[part, :] += dot(grad_hidden, up_weight[...], NT)
    grad_bias[...] = bias
    grad_up[...] = dot(turned[...], hiddens[...]).astype(grad_up.dtype)
    grad_down[...] = dot(actives[...], cotangent[...], (((0,), (0,)), ((), ()))).astype(grad_down.dtype)

    @pl.when(place == count - 1)
    def _():
        sums = [jnp.zeros((1, tokens.shape[1]), jnp.float32) for _ in range(4)]
        for part in parts:
            result[part, :] = total[part, :].astype(result.dtype)
            unit, inverse = units(middle[part, :])
            incoming = back[part, :]
            wide = cotangent[part, :].astype(jnp.float32)
            grad = wide + norm_pull(incoming, unit, inverse, vectors[5:6, :])
            grad_middle[part, :] = grad
            branch = grad.astype(jnp.bfloat16)
            turned[:, part] = mixed[part, :].T
            hiddens_low = dot(branch, out_weight[...], NT).astype(jnp.bfloat16)
            grad_mixed[part, :] = hiddens_low
            product = hiddens_low.astype(jnp.float32) * mixed[part, :].astype(jnp.float32)
            delta[part, :] = head_sums(product)
            normed[part, :] = branch
            sums[0] += row_sum(branch.astype(jnp.float32))
            sums[1] += row_sum(incoming * unit)
            sums[2] += row_sum(incoming)
            sums[3] += row_sum(wide)
        grad_out[...] = dot(turned[...], normed[...]).astype(grad_out.dtype)
        grad_rows[...] = jnp.concatenate(sums + [jnp.zeros((4, tokens.shape[1]), jnp.float32)], axis=0)


def head_sums(product):
    rows, width = product.shape
    lane = lax.broadcasted_iota(jnp.int32, (rows, LANE), 1)
    table = jnp.zeros((rows, LANE), jnp.float32)
    for pair in range(width // LANE):
        piece = product[:, pair * LANE : (pair + 1) * LANE]
        first = jnp.sum(jnp.where(lane < HD, piece, 0.0), axis=1, keepdims=True)
        second = jnp.sum(jnp.where(lane >= HD, piece, 0.0), axis=1, keepdims=True)
        table = jnp.where(lane == 2 * pair, first, table)
        table = jnp.where(lane == 2 * pair + 1, second, table)
    return table


def middle_block(tokens, mixed, cotangent, vectors, up_bias, out_weight, up_weight, down_weight, tile, chunk):
    rows, width = tokens.shape
    hidden = up_weight.shape[1]
    whole = lambda shape: pl.BlockSpec(shape, lambda i: (0,) * len(shape))
    across = lambda r: pl.BlockSpec((r, chunk), lambda i: (0, i))
    down = lambda: pl.BlockSpec((chunk, width), lambda i: (i, 0))
    full = (rows, width)
    return pl.pallas_call(
        functools.partial(middle_kernel, tile),
        grid=(hidden // chunk,),
        in_specs=[whole(full), whole(full), whole(full), whole(vectors.shape), across(1), whole((width, width)), across(width), down()],
        out_specs=[whole(full), whole(full), whole(full), whole((rows, LANE)), whole((width, width)), across(width), down(), whole((8, width)), across(1)],
        out_shape=[
            jax.ShapeDtypeStruct(full, jnp.bfloat16),
            jax.ShapeDtypeStruct(full, jnp.float32),
            jax.ShapeDtypeStruct(full, jnp.bfloat16),
            jax.ShapeDtypeStruct((rows, LANE), jnp.float32),
            jax.ShapeDtypeStruct((width, width), jnp.bfloat16),
            jax.ShapeDtypeStruct((width, hidden), jnp.bfloat16),
            jax.ShapeDtypeStruct((hidden, width), jnp.bfloat16),
            jax.ShapeDtypeStruct((8, width), jnp.float32),
            jax.ShapeDtypeStruct((1, hidden), jnp.float32),
        ],
        scratch_shapes=[
            pltpu.VMEM(full, jnp.float32),
            pltpu.VMEM(full, jnp.bfloat16),
            pltpu.VMEM((width, rows), jnp.bfloat16),
            pltpu.VMEM(full, jnp.float32),
            pltpu.VMEM(full, jnp.float32),
            pltpu.VMEM((rows, chunk), jnp.bfloat16),
            pltpu.VMEM((rows, chunk), jnp.bfloat16),
        ],
        name="middle",
    )(tokens, mixed, cotangent, vectors, up_bias, out_weight, up_weight, down_weight)


def last_kernel(tile, tokens, grad_middle, grad_query, grad_keys, grad_values, vectors, weights,
                grad_tokens, grad_qkv, grad_rows, turned):
    rows, width = tokens.shape
    sums = [jnp.zeros((1, width), jnp.float32) for _ in range(4)]
    for first in range(0, rows, tile):
        part = slice(first, first + tile)
        unit, inverse = units(tokens[part, :].astype(jnp.float32))
        turned[:, part] = (unit * vectors[0:1, :] + vectors[1:2, :]).astype(jnp.bfloat16).T
        incoming = dot(grad_query[part, :], weights[0], NT)
        incoming += dot(grad_keys[part, :], weights[1], NT)
        incoming += dot(grad_values[part, :], weights[2], NT)
        grad_tokens[part, :] = grad_middle[part, :] + norm_pull(incoming, unit, inverse, vectors[0:1, :])
        sums[0] += row_sum(incoming * unit)
        sums[1] += row_sum(incoming)
        sums[2] += row_sum(grad_query[part, :].astype(jnp.float32))
        sums[3] += row_sum(grad_values[part, :].astype(jnp.float32))
    for place, grad in enumerate((grad_query, grad_keys, grad_values)):
        grad_qkv[place] = dot(turned[...], grad[...]).astype(grad_qkv.dtype)
    grad_rows[...] = jnp.concatenate(sums + [jnp.zeros((4, width), jnp.float32)], axis=0)


def last_block(tokens, grad_middle, grad_query, grad_keys, grad_values, vectors, weights, tile):
    rows, width = tokens.shape
    return pl.pallas_call(
        functools.partial(last_kernel, tile),
        out_shape=[
            jax.ShapeDtypeStruct((rows, width), jnp.float32),
            jax.ShapeDtypeStruct(weights.shape, jnp.bfloat16),
            jax.ShapeDtypeStruct((8, width), jnp.float32),
        ],
        scratch_shapes=[pltpu.VMEM((width, rows), jnp.bfloat16)],
        name="last",
    )(tokens, grad_middle, grad_query, grad_keys, grad_values, vectors, weights)


def adamw_step(master, gradient, first_moment, second_moment):
    first_new = beta_one * first_moment + (1.0 - beta_one) * gradient
    second_new = beta_two * second_moment + (1.0 - beta_two) * gradient * gradient
    fix_one = 1.0 - beta_one**STEP
    fix_two = 1.0 - beta_two**STEP
    update = -learn_rate * (
        first_new / fix_one / (jnp.sqrt(second_new / fix_two) + adam_eps) + weight_decay * master
    )
    return (update, first_new, second_new)


def per_device(
    tokens,
    cotangent,
    clip_start,
    clip_end,
    qkv_weight,
    out_weight,
    up_weight,
    down_weight,
    vectors,
    qkv_first,
    out_first,
    up_first,
    down_first,
    vector_first,
    qkv_second,
    out_second,
    up_second,
    down_second,
    vector_second,
):
    rows, width = tokens.shape
    device = lax.axis_index("dev")
    devices = lax.axis_size("dev")
    heads = width // HD
    reach = (rows + CLIP - 2) // rows
    base = reach * rows
    window_first = device * rows - base
    shards = (qkv_weight, out_weight, up_weight, down_weight, vectors)
    low = [shard.astype(jnp.bfloat16) for shard in shards]
    qkv_full = lax.all_gather(low[0], "dev", axis=1, tiled=True)
    out_full = lax.all_gather(low[1], "dev", axis=0, tiled=True)
    up_full = lax.all_gather(low[2], "dev", axis=0, tiled=True)
    down_full = lax.all_gather(low[3], "dev", axis=0, tiled=True)
    vector_full = lax.all_gather(low[4], "dev", axis=1, tiled=True).astype(jnp.float32)

    offsets = [offset for offset in range(-reach, reach + 1)]
    spans = jnp.stack([clip_start, clip_end])

    def windowed(value):
        return [value if offset == 0 else shifted(value, "dev", -offset) for offset in offsets]

    tokens_window = jnp.concatenate(windowed(tokens), axis=0)
    spans_window = jnp.concatenate(windowed(spans), axis=1)
    places = window_first + jnp.arange(spans_window.shape[1], dtype=jnp.int32)
    inside = (places >= 0) & (places < devices * rows)
    starts = jnp.where(inside, spans_window[0] - window_first, FAR)
    ends = jnp.where(inside, spans_window[1] - window_first, 0)
    own_start, own_end = clip_start - window_first, clip_end - window_first

    tq, tk = FORWARD_TILES
    forward_bounds = jnp.stack([own_start[::tq] // tk, (own_end[tq - 1 :: tq] + tk - 1) // tk], axis=1).reshape(-1)
    rq, rk = QUERY_TILES
    query_bounds = jnp.stack([own_start[::rq] // rk, (own_end[rq - 1 :: rq] + rk - 1) // rk], axis=1).reshape(-1)
    sk, sq = KEY_TILES
    last_keys = base + sk - 1 + jnp.arange(rows // sk, dtype=jnp.int32) * sk
    last_tiles = jnp.sum((starts[::sq][None, :] <= last_keys[:, None]).astype(jnp.int32), axis=1)
    first_tiles = own_start[::sk] // sq
    last_tiles = first_tiles + jnp.sum(((starts[::sq][None, :] <= last_keys[:, None]) & (jnp.arange(starts.shape[0] // sq)[None, :] >= first_tiles[:, None])).astype(jnp.int32), axis=1)
    key_bounds = jnp.stack([first_tiles, last_tiles], axis=1).reshape(-1)
    needed = jnp.stack([own_start[0] // PROJECT_TILE, (jnp.sum((inside & (starts < base + rows)).astype(jnp.int32)) + jnp.maximum(-window_first, 0) + PROJECT_TILE - 1) // PROJECT_TILE])

    query_window, key_window, value_window = project(tokens_window, vector_full, qkv_full, needed, PROJECT_TILE)
    own = lambda value: lax.slice_in_dim(value, base, base + rows, axis=0)
    query = own(query_window)
    lower, upper = own_start[:, None], own_end[:, None]
    mixed, lse = attend(query, key_window, value_window, lower, upper, forward_bounds, tq, tk, GROUP)
    up_bias = vector_full[8:].reshape(1, -1)
    (result, grad_middle, grad_mixed, delta, grad_out, grad_up, grad_down, middle_rows, bias_row) = middle_block(
        tokens, mixed, cotangent, vector_full, up_bias, out_full, up_full, down_full, MIDDLE_TILE, MIDDLE_CHUNK
    )
    table = jnp.concatenate([lse[:, :heads], delta[:, :heads]], axis=1).T
    grad_window = jnp.concatenate(windowed(grad_mixed), axis=0)
    table_window = jnp.concatenate(windowed(table), axis=1)
    groups = heads // (2 * GROUP)
    lse_window = table_window[:heads].reshape(groups, 2 * GROUP, -1)
    delta_window = table_window[heads:].reshape(groups, 2 * GROUP, -1)
    grad_query = query_grad(query, grad_mixed, key_window, value_window, lse, delta, lower, upper, query_bounds, rq, rk, GROUP)
    grad_keys, grad_values = key_grad(
        own(key_window), own(value_window), query_window, grad_window, lse_window, delta_window,
        starts[None, :], ends[None, :], key_bounds, base, sk, sq, GROUP,
    )
    grad_tokens, grad_qkv, last_rows = last_block(
        tokens, grad_middle, grad_query, grad_keys, grad_values, vector_full, qkv_full, LAST_TILE
    )
    grad_vectors = jnp.concatenate([last_rows[:4], middle_rows[:4], bias_row.reshape(-1, width)], axis=0)
    owned = (
        lax.psum_scatter(grad_qkv, "dev", scatter_dimension=1, tiled=True).astype(jnp.float32),
        lax.psum_scatter(grad_out, "dev", scatter_dimension=0, tiled=True).astype(jnp.float32),
        lax.psum_scatter(grad_up, "dev", scatter_dimension=0, tiled=True).astype(jnp.float32),
        lax.psum_scatter(grad_down, "dev", scatter_dimension=0, tiled=True).astype(jnp.float32),
        lax.psum_scatter(grad_vectors, "dev", scatter_dimension=1, tiled=True),
    )
    firsts = (qkv_first, out_first, up_first, down_first, vector_first)
    seconds = (qkv_second, out_second, up_second, down_second, vector_second)
    stepped = [adamw_step(*four) for four in zip(shards, owned, firsts, seconds)]
    return (result, grad_tokens) + tuple(stepped[place][kind] for kind in range(3) for place in range(5))


def solution(mesh):
    in_specs = (
        P("dev", None),
        P("dev", None),
        P("dev"),
        P("dev"),
        P(None, "dev", None),
        P("dev", None),
        P("dev", None),
        P("dev", None),
        P(None, "dev"),
        P(None, "dev", None),
        P("dev", None),
        P("dev", None),
        P("dev", None),
        P(None, "dev"),
        P(None, "dev", None),
        P("dev", None),
        P("dev", None),
        P("dev", None),
        P(None, "dev"),
    )
    out_specs = (
        P("dev", None),
        P("dev", None),
        P(None, "dev", None),
        P("dev", None),
        P("dev", None),
        P("dev", None),
        P(None, "dev"),
        P(None, "dev", None),
        P("dev", None),
        P("dev", None),
        P("dev", None),
        P(None, "dev"),
        P(None, "dev", None),
        P("dev", None),
        P("dev", None),
        P("dev", None),
        P(None, "dev"),
    )
    return jax.shard_map(
        per_device, mesh=mesh, in_specs=in_specs, out_specs=out_specs, check_vma=False
    )
```

```python
import functools

import jax
import jax.numpy as jnp
from jax import lax
from jax.experimental import pallas as pl
from jax.experimental.pallas import tpu as pltpu
from jax.sharding import PartitionSpec as P

HD = 64
CLIP = 1500
STEP = 10
LANE = 128
FAR = 1 << 30
SQRT_HALF = 0.7071067811865476
INV_SQRT_TWO_PI = 0.3989422804014327


beta_one = 0.9
beta_two = 0.999
learn_rate = 0.02
weight_decay = 0.1
adam_eps = 1e-08
norm_eps = 1e-05
masked_score = -1e30
FORWARD_TILES = (256, 384)
QUERY_TILES = (256, 256)
KEY_TILES = (256, 256)
PROJECT_TILE = 768
MIDDLE_TILE = 256
MIDDLE_CHUNK = 512
LAST_TILE = 256
GROUP = 2
CHUNK_BYTES = 40000
PER_STEP = 4
HALO_START = 0
HALO_PASS = 3
GATHER_ORDERS = ((0, 1, 2), (0, 2, 1))
SCATTER_ORDERS = ((2, 1, 0), (1, 2, 0))
NT = (((1,), (1,)), ((), ()))
NN = (((1,), (0,)), ((), ()))


def shifted(value, axis, steps):
    count = lax.axis_size(axis)
    initial, last = (max(0, -steps), min(count, count - steps))
    return lax.ppermute(value, axis, [(source, source + steps) for source in range(initial, last)])


def dot(a, b, dims=NN):
    return lax.dot_general(a, b, dims, preferred_element_type=jnp.float32)


def stacked(pair, scale):
    lane = lax.broadcasted_iota(jnp.int32, pair.shape, 1)
    zero = jnp.zeros_like(pair)
    if scale is not None:
        pair = pair * jnp.asarray(scale, pair.dtype)
    return jnp.concatenate([jnp.where(lane < HD, pair, zero), jnp.where(lane >= HD, pair, zero)], axis=0)


def unstacked(both):
    rows = both.shape[0] // 2
    lane = lax.broadcasted_iota(jnp.int32, (rows, LANE), 1)
    return jnp.where(lane < HD, both[:rows], both[rows:])


def column(table, place):
    lane = lax.broadcasted_iota(jnp.int32, table.shape, 1)
    return jnp.sum(jnp.where(lane == place, table, 0.0), axis=1, keepdims=True)


def forward_kernel(tq, tk, pairs, bounds, lower, upper, q_ref, k_ref, v_ref, o_ref, lse_ref, qs, peak, acc):
    group = pl.program_id(0)
    tiles = q_ref.shape[0] // tq
    ones = jnp.ones((tk, LANE), jnp.bfloat16)

    @pl.when(group == 0)
    def _():
        lse_ref[...] = jnp.zeros_like(lse_ref)

    def one_tile(tile, none):
        rows = pl.ds(pl.multiple_of(tile * tq, tq), tq)
        for pair in range(pairs):
            qs[pair] = stacked(q_ref[rows, pair * LANE : (pair + 1) * LANE], HD ** -0.5)
        peak[...] = jnp.full_like(peak, masked_score)
        acc[...] = jnp.zeros_like(acc)
        low, high = lower[rows, :], upper[rows, :]

        def step(key_tile, none):
            first = pl.multiple_of(key_tile * tk, tk)
            places = first + lax.broadcasted_iota(jnp.int32, (tq, tk), 1)
            bias = jnp.where((places >= low) & (places < high), 0.0, masked_score)
            bias = jnp.concatenate([bias, bias], axis=0)
            for pair in range(pairs):
                lanes = slice(pair * LANE, (pair + 1) * LANE)
                scores = dot(qs[pair], k_ref[pl.ds(first, tk), lanes], NT) + bias
                old = peak[pair]
                new = jnp.maximum(old, jnp.max(scores, axis=1, keepdims=True))
                peak[pair] = new
                weights = jnp.exp(scores - new[:, :1]).astype(jnp.bfloat16)
                values = jnp.concatenate([v_ref[pl.ds(first, tk), lanes], ones], axis=1)
                scale = jnp.exp(old - new)
                acc[pair] = acc[pair] * jnp.concatenate([scale, scale], axis=1) + dot(weights, values)
            return none

        lax.fori_loop(bounds[2 * tile], bounds[2 * tile + 1], step, 0)
        lane = lax.broadcasted_iota(jnp.int32, (tq, LANE), 1)
        table = lse_ref[rows, :]
        for pair in range(pairs):
            both = acc[pair]
            total = both[:, LANE:]
            o_ref[rows, pair * LANE : (pair + 1) * LANE] = unstacked(both[:, :LANE] / total).astype(o_ref.dtype)
            logs = peak[pair] + jnp.log(total)
            head = (group * pairs + pair) * 2
            table = jnp.where(lane == head, logs[:tq], table)
            table = jnp.where(lane == head + 1, logs[tq:], table)
        lse_ref[rows, :] = table
        return none

    lax.fori_loop(0, tiles, one_tile, 0)


def attend(query, keys, values, lower, upper, bounds, tq, tk, pairs):
    rows, width = query.shape
    window = keys.shape[0]
    lanes = pairs * LANE
    return pl.pallas_call(
        functools.partial(forward_kernel, tq, tk, pairs),
        grid_spec=pltpu.PrefetchScalarGridSpec(
            num_scalar_prefetch=1, grid=(width // lanes,),
            in_specs=[
                pl.BlockSpec((rows, 1), lambda g, b: (0, 0)),
                pl.BlockSpec((rows, 1), lambda g, b: (0, 0)),
                pl.BlockSpec((rows, lanes), lambda g, b: (0, g)),
                pl.BlockSpec((window, lanes), lambda g, b: (0, g)),
                pl.BlockSpec((window, lanes), lambda g, b: (0, g)),
            ],
            out_specs=[pl.BlockSpec((rows, lanes), lambda g, b: (0, g)), pl.BlockSpec((rows, LANE), lambda g, b: (0, 0))],
            scratch_shapes=[
                pltpu.VMEM((pairs, 2 * tq, LANE), jnp.bfloat16),
                pltpu.VMEM((pairs, 2 * tq, LANE), jnp.float32),
                pltpu.VMEM((pairs, 2 * tq, 2 * LANE), jnp.float32),
            ],
        ),
        out_shape=[jax.ShapeDtypeStruct((rows, width), jnp.bfloat16), jax.ShapeDtypeStruct((rows, LANE), jnp.float32)],
        name="attend",
    )(bounds, lower, upper, query, keys, values)


def query_grad_kernel(tq, tk, pairs, bounds, lower, upper, q_ref, g_ref, k_ref, v_ref, lse_ref, delta_ref, dq_ref, qs, gs, logs, deltas, acc):
    group = pl.program_id(0)
    tiles = q_ref.shape[0] // tq

    def one_tile(tile, none):
        rows = pl.ds(pl.multiple_of(tile * tq, tq), tq)
        table, other = lse_ref[rows, :], delta_ref[rows, :]
        for pair in range(pairs):
            lanes = slice(pair * LANE, (pair + 1) * LANE)
            qs[pair] = stacked(q_ref[rows, lanes], HD ** -0.5)
            gs[pair] = stacked(g_ref[rows, lanes], None)
            head = (group * pairs + pair) * 2
            logs[pair] = jnp.broadcast_to(jnp.concatenate([column(table, head), column(table, head + 1)], axis=0), logs.shape[1:])
            deltas[pair] = jnp.broadcast_to(jnp.concatenate([column(other, head), column(other, head + 1)], axis=0), logs.shape[1:])
        acc[...] = jnp.zeros_like(acc)
        low, high = lower[rows, :], upper[rows, :]

        def step(key_tile, none):
            first = pl.multiple_of(key_tile * tk, tk)
            places = first + lax.broadcasted_iota(jnp.int32, (tq, tk), 1)
            bias = jnp.where((places >= low) & (places < high), 0.0, masked_score)
            bias = jnp.concatenate([bias, bias], axis=0)
            for pair in range(pairs):
                lanes = slice(pair * LANE, (pair + 1) * LANE)
                keys = k_ref[pl.ds(first, tk), lanes]
                scores = dot(qs[pair], keys, NT) + bias
                probs = jnp.exp(scores - logs[pair][:, :1])
                grad_probs = dot(gs[pair], v_ref[pl.ds(first, tk), lanes], NT)
                grad_scores = (probs * (grad_probs - deltas[pair][:, :1])).astype(jnp.bfloat16)
                acc[pair] += dot(grad_scores, keys)
            return none

        lax.fori_loop(bounds[2 * tile], bounds[2 * tile + 1], step, 0)
        for pair in range(pairs):
            dq_ref[rows, pair * LANE : (pair + 1) * LANE] = (unstacked(acc[pair]) * HD ** -0.5).astype(dq_ref.dtype)
        return none

    lax.fori_loop(0, tiles, one_tile, 0)


def query_grad(query, grad, keys, values, lse, delta, lower, upper, bounds, tq, tk, pairs):
    rows, width = query.shape
    window = keys.shape[0]
    lanes = pairs * LANE
    own = lambda: pl.BlockSpec((rows, lanes), lambda g, b: (0, g))
    far = lambda: pl.BlockSpec((window, lanes), lambda g, b: (0, g))
    fixed = lambda cols: pl.BlockSpec((rows, cols), lambda g, b: (0, 0))
    return pl.pallas_call(
        functools.partial(query_grad_kernel, tq, tk, pairs),
        grid_spec=pltpu.PrefetchScalarGridSpec(
            num_scalar_prefetch=1, grid=(width // lanes,),
            in_specs=[fixed(1), fixed(1), own(), own(), far(), far(), fixed(LANE), fixed(LANE)],
            out_specs=own(),
            scratch_shapes=[
                pltpu.VMEM((pairs, 2 * tq, LANE), jnp.bfloat16),
                pltpu.VMEM((pairs, 2 * tq, LANE), jnp.bfloat16),
                pltpu.VMEM((pairs, 2 * tq, LANE), jnp.float32),
                pltpu.VMEM((pairs, 2 * tq, LANE), jnp.float32),
                pltpu.VMEM((pairs, 2 * tq, LANE), jnp.float32),
            ],
        ),
        out_shape=jax.ShapeDtypeStruct((rows, width), jnp.bfloat16),
        name="query_grad",
    )(bounds, lower, upper, query, grad, keys, values, lse, delta)


def key_grad_kernel(tk, tq, pairs, base, bounds, lower, upper, k_ref, v_ref, q_ref, g_ref, lse_ref, delta_ref, dk_ref, dv_ref, ks, vs, acc):
    tiles = k_ref.shape[0] // tk

    def one_tile(tile, none):
        rows = pl.ds(pl.multiple_of(tile * tk, tk), tk)
        for pair in range(pairs):
            lanes = slice(pair * LANE, (pair + 1) * LANE)
            ks[pair] = stacked(k_ref[rows, lanes], HD ** -0.5)
            vs[pair] = stacked(v_ref[rows, lanes], None)
        acc[...] = jnp.zeros_like(acc)

        def step(query_tile, none):
            first = pl.multiple_of(query_tile * tq, tq)
            here = pl.ds(first, tq)
            places = base + tile * tk + lax.broadcasted_iota(jnp.int32, (tk, tq), 0)
            bias = jnp.where((places >= lower[:, here]) & (places < upper[:, here]), 0.0, masked_score)
            for pair in range(pairs):
                lanes = slice(pair * LANE, (pair + 1) * LANE)
                queries, grads = q_ref[here, lanes], g_ref[here, lanes]
                scores = dot(ks[pair], queries, NT)
                grad_probs = dot(vs[pair], grads, NT)
                probs, grad_scores = [], []
                for half in range(2):
                    part = slice(half * tk, (half + 1) * tk)
                    head = slice(2 * pair + half, 2 * pair + half + 1)
                    prob = jnp.exp(scores[part] + bias - lse_ref[0, head, here])
                    probs.append(prob.astype(jnp.bfloat16))
                    grad_scores.append((prob * (grad_probs[part] - delta_ref[0, head, here])).astype(jnp.bfloat16))
                acc[pair, :, :LANE] += dot(jnp.concatenate(grad_scores, axis=0), queries)
                acc[pair, :, LANE:] += dot(jnp.concatenate(probs, axis=0), grads)
            return none

        lax.fori_loop(bounds[2 * tile], bounds[2 * tile + 1], step, 0)
        for pair in range(pairs):
            lanes = slice(pair * LANE, (pair + 1) * LANE)
            dk_ref[rows, lanes] = (unstacked(acc[pair, :, :LANE]) * HD ** -0.5).astype(dk_ref.dtype)
            dv_ref[rows, lanes] = unstacked(acc[pair, :, LANE:]).astype(dv_ref.dtype)
        return none

    lax.fori_loop(0, tiles, one_tile, 0)


def key_grad(keys, values, query, grad, lse, delta, lower, upper, bounds, base, tk, tq, pairs):
    rows, width = keys.shape
    window = query.shape[0]
    lanes = pairs * LANE
    own = lambda: pl.BlockSpec((rows, lanes), lambda g, b: (0, g))
    far = lambda: pl.BlockSpec((window, lanes), lambda g, b: (0, g))
    line = lambda: pl.BlockSpec((1, window), lambda g, b: (0, 0))
    heads = lambda: pl.BlockSpec((1, 2 * pairs, window), lambda g, b: (g, 0, 0))
    return pl.pallas_call(
        functools.partial(key_grad_kernel, tk, tq, pairs, base),
        grid_spec=pltpu.PrefetchScalarGridSpec(
            num_scalar_prefetch=1, grid=(width // lanes,),
            in_specs=[line(), line(), own(), own(), far(), far(), heads(), heads()],
            out_specs=[own(), own()],
            scratch_shapes=[
                pltpu.VMEM((pairs, 2 * tk, LANE), jnp.bfloat16),
                pltpu.VMEM((pairs, 2 * tk, LANE), jnp.bfloat16),
                pltpu.VMEM((pairs, 2 * tk, 2 * LANE), jnp.float32),
            ],
        ),
        out_shape=[jax.ShapeDtypeStruct((rows, width), jnp.bfloat16)] * 2,
        name="key_grad",
    )(bounds, lower, upper, keys, values, query, grad, lse, delta)


def units(values):
    centre = values - jnp.mean(values, axis=-1, keepdims=True)
    inverse = lax.rsqrt(jnp.mean(centre * centre, axis=-1, keepdims=True) + norm_eps)
    return centre * inverse, inverse


def norm_pull(grad_output, unit, inverse, gain):
    grad_unit = grad_output * gain
    first = jnp.mean(grad_unit, axis=-1, keepdims=True)
    second = jnp.mean(grad_unit * unit, axis=-1, keepdims=True)
    return inverse * (grad_unit - first - unit * second)


def row_sum(values):
    return jnp.sum(values, axis=0, keepdims=True)


def gelu_pair(hidden):
    inner = 0.5 + 0.5 * lax.erf(hidden * SQRT_HALF)
    slope = inner + hidden * (jnp.exp(-0.5 * hidden * hidden) * INV_SQRT_TWO_PI)
    return hidden * inner, slope


def project_kernel(tile, active, tokens, vectors, weights, query, keys, values):
    place = pl.program_id(0)
    needed = (place >= active[0]) & (place < active[1])

    @pl.when(needed)
    def _():
        unit = units(tokens[...].astype(jnp.float32))[0]
        normed = (unit * vectors[0:1, :] + vectors[1:2, :]).astype(jnp.bfloat16)
        query[...] = (dot(normed, weights[0]) + vectors[2:3, :]).astype(query.dtype)
        keys[...] = dot(normed, weights[1]).astype(keys.dtype)
        values[...] = (dot(normed, weights[2]) + vectors[3:4, :]).astype(values.dtype)

    @pl.when(jnp.logical_not(needed))
    def _():
        for out in (query, keys, values):
            out[...] = jnp.zeros_like(out)


def project(tokens, vectors, weights, active, tile):
    rows, width = tokens.shape
    block = lambda: pl.BlockSpec((tile, width), lambda i, b: (i, 0))
    return pl.pallas_call(
        functools.partial(project_kernel, tile),
        grid_spec=pltpu.PrefetchScalarGridSpec(
            num_scalar_prefetch=1, grid=(rows // tile,),
            in_specs=[
                block(),
                pl.BlockSpec(vectors.shape, lambda i, b: (0, 0)),
                pl.BlockSpec(weights.shape, lambda i, b: (0, 0, 0)),
            ],
            out_specs=[block(), block(), block()],
        ),
        out_shape=[jax.ShapeDtypeStruct((rows, width), jnp.bfloat16)] * 3,
        name="project",
    )(active, tokens, vectors, weights)


def middle_kernel(tile, tokens, mixed, cotangent, vectors, up_bias, out_weight, up_weight, down_weight,
                  result, grad_middle, grad_mixed, delta, grad_out, grad_up, grad_down, grad_rows, grad_bias,
                  middle, normed, turned, total, back, actives, hiddens):
    place, count = pl.program_id(0), pl.num_programs(0)
    rows = tokens.shape[0]
    parts = [slice(i, i + tile) for i in range(0, rows, tile)]

    @pl.when(place == 0)
    def _():
        for part in parts:
            branch = dot(mixed[part, :], out_weight[...]) + vectors[4:5, :]
            wide = tokens[part, :].astype(jnp.float32) + branch
            middle[part, :] = wide
            unit = units(wide)[0]
            low = (unit * vectors[5:6, :] + vectors[6:7, :]).astype(jnp.bfloat16)
            normed[part, :] = low
            turned[:, part] = low.T
            total[part, :] = wide + vectors[7:8, :]
        back[...] = jnp.zeros_like(back)

    bias = jnp.zeros_like(grad_bias)
    for part in parts:
        hidden = dot(normed[part, :], up_weight[...]) + up_bias[...]
        wide, slope = gelu_pair(hidden)
        active = wide.astype(jnp.bfloat16)
        grad_active = dot(cotangent[part, :], down_weight[...], NT)
        grad_hidden = (grad_active * slope).astype(jnp.bfloat16)
        actives[part, :] = active
        hiddens[part, :] = grad_hidden
        bias += row_sum(grad_hidden.astype(jnp.float32))
        total[part, :] += dot(active, down_weight[...])
        back[part, :] += dot(grad_hidden, up_weight[...], NT)
    grad_bias[...] = bias
    grad_up[...] = dot(turned[...], hiddens[...]).astype(grad_up.dtype)
    grad_down[...] = dot(actives[...], cotangent[...], (((0,), (0,)), ((), ()))).astype(grad_down.dtype)

    @pl.when(place == count - 1)
    def _():
        sums = [jnp.zeros((1, tokens.shape[1]), jnp.float32) for _ in range(4)]
        for part in parts:
            result[part, :] = total[part, :].astype(result.dtype)
            unit, inverse = units(middle[part, :])
            incoming = back[part, :]
            wide = cotangent[part, :].astype(jnp.float32)
            grad = wide + norm_pull(incoming, unit, inverse, vectors[5:6, :])
            grad_middle[part, :] = grad
            branch = grad.astype(jnp.bfloat16)
            turned[:, part] = mixed[part, :].T
            hiddens_low = dot(branch, out_weight[...], NT).astype(jnp.bfloat16)
            grad_mixed[part, :] = hiddens_low
            product = hiddens_low.astype(jnp.float32) * mixed[part, :].astype(jnp.float32)
            delta[part, :] = head_sums(product)
            normed[part, :] = branch
            sums[0] += row_sum(branch.astype(jnp.float32))
            sums[1] += row_sum(incoming * unit)
            sums[2] += row_sum(incoming)
            sums[3] += row_sum(wide)
        grad_out[...] = dot(turned[...], normed[...]).astype(grad_out.dtype)
        grad_rows[...] = jnp.concatenate(sums + [jnp.zeros((4, tokens.shape[1]), jnp.float32)], axis=0)


def head_sums(product):
    rows, width = product.shape
    lane = lax.broadcasted_iota(jnp.int32, (rows, LANE), 1)
    table = jnp.zeros((rows, LANE), jnp.float32)
    for pair in range(width // LANE):
        piece = product[:, pair * LANE : (pair + 1) * LANE]
        first = jnp.sum(jnp.where(lane < HD, piece, 0.0), axis=1, keepdims=True)
        second = jnp.sum(jnp.where(lane >= HD, piece, 0.0), axis=1, keepdims=True)
        table = jnp.where(lane == 2 * pair, first, table)
        table = jnp.where(lane == 2 * pair + 1, second, table)
    return table


def middle_block(tokens, mixed, cotangent, vectors, up_bias, out_weight, up_weight, down_weight, tile, chunk):
    rows, width = tokens.shape
    hidden = up_weight.shape[1]
    whole = lambda shape: pl.BlockSpec(shape, lambda i: (0,) * len(shape))
    across = lambda r: pl.BlockSpec((r, chunk), lambda i: (0, i))
    down = lambda: pl.BlockSpec((chunk, width), lambda i: (i, 0))
    full = (rows, width)
    return pl.pallas_call(
        functools.partial(middle_kernel, tile),
        grid=(hidden // chunk,),
        in_specs=[whole(full), whole(full), whole(full), whole(vectors.shape), across(1), whole((width, width)), across(width), down()],
        out_specs=[whole(full), whole(full), whole(full), whole((rows, LANE)), whole((width, width)), across(width), down(), whole((8, width)), across(1)],
        out_shape=[
            jax.ShapeDtypeStruct(full, jnp.bfloat16),
            jax.ShapeDtypeStruct(full, jnp.float32),
            jax.ShapeDtypeStruct(full, jnp.bfloat16),
            jax.ShapeDtypeStruct((rows, LANE), jnp.float32),
            jax.ShapeDtypeStruct((width, width), jnp.bfloat16),
            jax.ShapeDtypeStruct((width, hidden), jnp.bfloat16),
            jax.ShapeDtypeStruct((hidden, width), jnp.bfloat16),
            jax.ShapeDtypeStruct((8, width), jnp.float32),
            jax.ShapeDtypeStruct((1, hidden), jnp.float32),
        ],
        scratch_shapes=[
            pltpu.VMEM(full, jnp.float32),
            pltpu.VMEM(full, jnp.bfloat16),
            pltpu.VMEM((width, rows), jnp.bfloat16),
            pltpu.VMEM(full, jnp.float32),
            pltpu.VMEM(full, jnp.float32),
            pltpu.VMEM((rows, chunk), jnp.bfloat16),
            pltpu.VMEM((rows, chunk), jnp.bfloat16),
        ],
        name="middle",
    )(tokens, mixed, cotangent, vectors, up_bias, out_weight, up_weight, down_weight)


def last_kernel(tile, tokens, grad_middle, grad_query, grad_keys, grad_values, vectors, weights,
                grad_tokens, grad_qkv, grad_rows, turned):
    rows, width = tokens.shape
    sums = [jnp.zeros((1, width), jnp.float32) for _ in range(4)]
    for first in range(0, rows, tile):
        part = slice(first, first + tile)
        unit, inverse = units(tokens[part, :].astype(jnp.float32))
        turned[:, part] = (unit * vectors[0:1, :] + vectors[1:2, :]).astype(jnp.bfloat16).T
        incoming = dot(grad_query[part, :], weights[0], NT)
        incoming += dot(grad_keys[part, :], weights[1], NT)
        incoming += dot(grad_values[part, :], weights[2], NT)
        grad_tokens[part, :] = grad_middle[part, :] + norm_pull(incoming, unit, inverse, vectors[0:1, :])
        sums[0] += row_sum(incoming * unit)
        sums[1] += row_sum(incoming)
        sums[2] += row_sum(grad_query[part, :].astype(jnp.float32))
        sums[3] += row_sum(grad_values[part, :].astype(jnp.float32))
    for place, grad in enumerate((grad_query, grad_keys, grad_values)):
        grad_qkv[place] = dot(turned[...], grad[...]).astype(grad_qkv.dtype)
    grad_rows[...] = jnp.concatenate(sums + [jnp.zeros((4, width), jnp.float32)], axis=0)


def last_block(tokens, grad_middle, grad_query, grad_keys, grad_values, vectors, weights, tile):
    rows, width = tokens.shape
    return pl.pallas_call(
        functools.partial(last_kernel, tile),
        out_shape=[
            jax.ShapeDtypeStruct((rows, width), jnp.float32),
            jax.ShapeDtypeStruct(weights.shape, jnp.bfloat16),
            jax.ShapeDtypeStruct((8, width), jnp.float32),
        ],
        scratch_shapes=[pltpu.VMEM((width, rows), jnp.bfloat16)],
        name="last",
    )(tokens, grad_middle, grad_query, grad_keys, grad_values, vectors, weights)


def chip_axes(devices):
    chips = devices // 2
    return {16: (4, 2, 2), 64: (4, 4, 4)}.get(chips, (chips, 1, 1))


class Place:
    def __init__(self, dims):
        self.dims = dims
        self.me = lax.axis_index("dev")
        self.core = lax.rem(self.me, 2)
        chip = self.me // 2
        self.at = (chip // (dims[1] * dims[2]), lax.rem(chip // dims[2], dims[1]), lax.rem(chip, dims[2]))
        self.partner = self.me + 1 - 2 * self.core

    def peer(self, axis, step):
        there = lax.rem(self.at[axis] + step, self.dims[axis])
        at = [there if a == axis else self.at[a] for a in range(3)]
        return ((at[0] * self.dims[1] + at[1]) * self.dims[2] + at[2]) * 2 + self.core, there

    def peers(self):
        return [self.partner] + [self.peer(axis, step)[0] for axis in range(3) for step in range(1, self.dims[axis])]


def remote(source, target, send, recv, device):
    return pltpu.make_async_remote_copy(
        src_ref=source, dst_ref=target, send_sem=send, recv_sem=recv,
        device_id=(device,), device_id_type=pl.DeviceIdType.MESH,
    )


def greet(peers, around=None, devices=0):
    barrier = pltpu.get_barrier_semaphore()
    count = len(peers)
    for peer in peers:
        pl.semaphore_signal(barrier, inc=1, device_id=(peer,), device_id_type=pl.DeviceIdType.MESH)
    if around is not None:
        for other in (around - 2, around + 2):
            there = (other >= 0) & (other < devices)
            count = count + there.astype(jnp.int32)

            @pl.when(there)
            def _():
                pl.semaphore_signal(barrier, inc=1, device_id=(other,), device_id_type=pl.DeviceIdType.MESH)

    pl.semaphore_wait(barrier, count)


class Halo:
    def __init__(self, place, devices, own, window, send, recv, local):
        self.place, self.devices, self.own, self.window = place, devices, own, window
        self.send, self.recv, self.local = send, recv, local
        me, core = place.me, place.core
        self.above, self.below = me + 2 < devices, me >= 2
        self.up = remote(own, window.at[0], send.at[0], recv.at[0], me + 2)
        self.down = remote(own, window.at[4], send.at[1], recv.at[1], me - 2)
        side = jnp.where(core == 0, 1, 3)
        self.across = remote(own, window.at[side], send.at[2], recv.at[2], place.partner)
        self.kept = jnp.where(core == 0, 4, 0)
        self.relay = remote(window.at[self.kept], window.at[4 - side], send.at[3], recv.at[3], place.partner)
        self.keep = pltpu.make_async_copy(own, window.at[2], local)

    def start(self):
        pl.when(self.above)(self.up.start)
        pl.when(self.below)(self.down.start)
        self.across.start()
        self.keep.start()

    def pass_on(self):
        pl.when(self.below)(self.up.wait_recv)
        pl.when(self.above)(self.down.wait_recv)
        even = self.place.core == 0
        self.relays = jnp.where(even, self.above, self.below)
        pl.when(self.relays)(self.relay.start)

    def finish(self):
        even = self.place.core == 0
        comes = jnp.where(even, self.below, self.above)
        self.across.wait_recv()
        pl.when(comes)(self.relay.wait_recv)
        self.keep.wait()
        pl.when(self.above)(self.up.wait_send)
        pl.when(self.below)(self.down.wait_send)
        self.across.wait_send()
        pl.when(self.relays)(self.relay.wait_send)


def gather_kernel(dims, devices, chunks, orders, arrays, halos, *refs):
    shards, owns = refs[:arrays], refs[arrays : arrays + halos]
    fulls = refs[arrays + halos : 2 * arrays + halos]
    windows = refs[2 * arrays + halos : 2 * (arrays + halos)]
    send, recv, local, halo_send, halo_recv, halo_local = refs[2 * (arrays + halos) :]
    place = Place(dims)
    greet(place.peers(), place.me, devices)
    parts = [
        Halo(place, devices, owns[i], windows[i], halo_send.at[i], halo_recv.at[i], halo_local.at[i])
        for i in range(halos)
    ]
    count = len(chunks)
    started = {}

    def stage(number, level):
        array, lead, lanes = chunks[number]
        shard, full = shards[array], fulls[array]
        front = () if lead is None else (lead,)
        source = shard.at[front + (slice(None), lanes)] if front else shard.at[:, lanes]
        order = orders[number]
        done = order[: min(level, 3)]
        index = tuple(slice(None) if axis in done else place.at[axis] for axis in range(3))
        view = lambda index, core: full.at[front + index + (core, slice(None), lanes)]
        if level == 0:
            mine = pltpu.make_async_copy(source, view(index, place.core), local.at[number])
            mine.start()
            started[number] = [mine]
        else:
            for copy in started[number, level - 1]:
                copy.wait_recv()
            if level == 1:
                started[number][0].wait()
            source = view(index, place.core)
        copies = []
        if level == 3:
            copies.append(remote(source, source, send.at[number, 0], recv.at[number, 0], place.partner))
        else:
            base = 1 + sum(dims[axis] - 1 for axis in order[:level])
            for step in range(1, dims[order[level]]):
                slot = base + step - 1
                device = place.peer(order[level], step)[0]
                target = view(index, place.core)
                copies.append(remote(source, target, send.at[number, slot], recv.at[number, slot], device))
        for copy in copies:
            copy.start()
        started[number, level] = copies

    steps = -(-count // PER_STEP)
    for time in range(steps + 3):
        for level in (3, 2, 1, 0):
            for number in range((time - level) * PER_STEP, (time - level + 1) * PER_STEP):
                if 0 <= number < count:
                    stage(number, level)
        if time == HALO_START:
            for part in parts:
                part.start()
        if time == min(HALO_PASS, steps + 2):
            for part in parts:
                part.pass_on()
    for number in range(count):
        for copy in started[number, 3]:
            copy.wait_recv()
        for level in range(4):
            for copy in started[number, level]:
                copy.wait_send()
    for part in parts:
        part.finish()


def gather(shards, owns, devices):
    dims = chip_axes(devices)
    chunks = []
    for array, shard in enumerate(shards):
        lanes = shard.shape[-1]
        if shard.ndim == 3:
            chunks += [(array, lead, slice(0, lanes)) for lead in range(shard.shape[0])]
        else:
            wide = min(lanes, max(CHUNK_BYTES // (2 * shard.shape[0]) // LANE * LANE, LANE))
            wide = max(w for w in range(LANE, wide + 1, LANE) if lanes % w == 0)
            chunks += [(array, None, slice(first, first + wide)) for first in range(0, lanes, wide)]
    orders = [GATHER_ORDERS[number % len(GATHER_ORDERS)] for number in range(len(chunks))]
    slots = 1 + sum(size - 1 for size in dims)
    anywhere = pl.BlockSpec(memory_space=pl.ANY)
    inside = pl.BlockSpec(memory_space=pltpu.VMEM)
    outs = [
        jax.ShapeDtypeStruct(shard.shape[:-2] + dims + (2,) + shard.shape[-2:], shard.dtype) for shard in shards
    ] + [jax.ShapeDtypeStruct((5,) + own.shape, own.dtype) for own in owns]
    done = pl.pallas_call(
        functools.partial(gather_kernel, dims, devices, chunks, orders, len(shards), len(owns)),
        in_specs=[inside] * (len(shards) + len(owns)),
        out_specs=[anywhere] * len(outs),
        out_shape=outs,
        scratch_shapes=[
            pltpu.SemaphoreType.DMA((len(chunks), slots)),
            pltpu.SemaphoreType.DMA((len(chunks), slots)),
            pltpu.SemaphoreType.DMA((len(chunks),)),
            pltpu.SemaphoreType.DMA((max(len(owns), 1), 4)),
            pltpu.SemaphoreType.DMA((max(len(owns), 1), 4)),
            pltpu.SemaphoreType.DMA((max(len(owns), 1),)),
        ],
        compiler_params=pltpu.CompilerParams(collective_id=0, has_side_effects=True),
        name="gather",
    )(*shards, *owns)
    return done[: len(shards)], done[len(shards) :]


def halo_kernel(dims, devices, halos, *refs):
    owns, windows = refs[:halos], refs[halos : 2 * halos]
    send, recv, local = refs[2 * halos :]
    place = Place(dims)
    greet([place.partner], place.me, devices)
    parts = [Halo(place, devices, owns[i], windows[i], send.at[i], recv.at[i], local.at[i]) for i in range(halos)]
    for part in parts:
        part.start()
    for part in parts:
        part.pass_on()
    for part in parts:
        part.finish()


def halo(owns, devices):
    outs = [jax.ShapeDtypeStruct((5,) + own.shape, own.dtype) for own in owns]
    return pl.pallas_call(
        functools.partial(halo_kernel, chip_axes(devices), devices, len(owns)),
        in_specs=[pl.BlockSpec(memory_space=pltpu.VMEM)] * len(owns),
        out_specs=[pl.BlockSpec(memory_space=pl.ANY)] * len(owns),
        out_shape=outs,
        scratch_shapes=[
            pltpu.SemaphoreType.DMA((len(owns), 4)),
            pltpu.SemaphoreType.DMA((len(owns), 4)),
            pltpu.SemaphoreType.DMA((len(owns),)),
        ],
        compiler_params=pltpu.CompilerParams(collective_id=1, has_side_effects=True),
        name="halo",
    )(*owns)


def scatter_kernel(dims, chunks, arrays, orders, *refs):
    grads, outs = refs[:arrays], refs[arrays : 2 * arrays]
    rest = refs[2 * arrays :]
    count = len(chunks)
    buffers = [rest[5 * i : 5 * i + 5] for i in range(count)]
    send, recv, local = rest[5 * count :]
    place = Place(dims)
    greet(place.peers())
    started = {}

    def source(number, core):
        array, lead, lanes = chunks[number]
        front = () if lead is None else (lead,)
        return grads[array].at[front + (slice(None), slice(None), slice(None), core, slice(None), lanes)]

    def spread(shape, one):
        total = 1
        for size in shape:
            total *= size

        def body(flat, none):
            index = []
            for size in reversed(shape):
                index.insert(0, lax.rem(flat, size))
                flat = flat // size
            one(tuple(index))
            return none

        lax.fori_loop(0, total, body, 0)

    def stage(number, level):
        own, first, second, third, fourth = buffers[number]
        order = orders[number]
        held = (own, second, third, fourth)
        copies = []
        if level == 0:
            mine = pltpu.make_async_copy(source(number, place.core), own, local.at[number])
            mine.start()
            started[number] = mine
            copies.append(remote(source(number, 1 - place.core), first, send.at[number, 0], recv.at[number, 0], place.partner))
        else:
            for copy in started[number, level - 1]:
                copy.wait_recv()
            remaining = [axis for axis in range(3) if axis not in order[: level - 1]]
            if level == 1:
                started[number].wait()

                def add(index):
                    total = own[index].astype(jnp.float32) + first[index].astype(jnp.float32)
                    own[index] = total.astype(own.dtype)

                spread(dims, add)
            else:
                combine(number, level)
            axis = order[level - 1]
            base = 1 + sum(dims[a] - 1 for a in order[: level - 1])
            for step in range(1, dims[axis]):
                device, there = place.peer(axis, step)
                where = tuple(there if a == axis else slice(None) for a in remaining)
                slot = base + step - 1
                piece = (own if level == 1 else held[level - 1].at[0]).at[where]
                copies.append(remote(piece, held[level].at[step - 1], send.at[number, slot], recv.at[number, slot], device))
        for copy in copies:
            copy.start()
        started[number, level] = copies

    def combine(number, level):
        own, first, second, third, fourth = buffers[number]
        order = orders[number]
        held = (own, second, third, fourth)
        axis = order[level - 2]
        before = [a for a in range(3) if a not in order[: level - 2]]
        after = [a for a in before if a != axis]
        slots = dims[axis] - 1
        old = own if level == 2 else held[level - 2].at[0]
        new = held[level - 1]
        array, lead, lanes = chunks[number]

        def add(index):
            where = list(index)
            where.insert(before.index(axis), place.at[axis])
            total = old[tuple(where)].astype(jnp.float32)
            for slot in range(slots):
                total += new[(slot,) + index].astype(jnp.float32)
            if level == 4:
                if lead is None:
                    outs[array][:, lanes] = total
                else:
                    outs[array][lead, :, lanes] = total
            else:
                new[(0,) + index] = total.astype(new.dtype)

        if after:
            spread([dims[a] for a in after], add)
        else:
            add(())

    for time in range(-(-count // PER_STEP) + 4):
        for level in (4, 3, 2, 1, 0):
            for number in range((time - level) * PER_STEP, (time - level + 1) * PER_STEP):
                if not 0 <= number < count:
                    continue
                if level == 4:
                    for copy in started[number, 3]:
                        copy.wait_recv()
                    combine(number, 4)
                else:
                    stage(number, level)
    for number in range(count):
        for level in range(4):
            for copy in started[number, level]:
                copy.wait_send()


def scatter(grads, devices):
    dims = chip_axes(devices)
    chunks = []
    for array, grad in enumerate(grads):
        rows, lanes = grad.shape[-2:]
        if grad.ndim == 7:
            chunks += [(array, lead, slice(0, lanes)) for lead in range(grad.shape[0])]
        else:
            wide = min(lanes, max(CHUNK_BYTES // (2 * rows) // LANE * LANE, LANE))
            wide = max(w for w in range(LANE, wide + 1, LANE) if lanes % w == 0)
            chunks += [(array, None, slice(first, first + wide)) for first in range(0, lanes, wide)]
    orders = [SCATTER_ORDERS[number % len(SCATTER_ORDERS)] for number in range(len(chunks))]
    scratch = []
    for (array, lead, lanes), order in zip(chunks, orders):
        grad = grads[array]
        piece = (grad.shape[-2], lanes.stop - lanes.start)
        left = [dims[a] for a in range(3)]
        scratch += [pltpu.VMEM(dims + piece, grad.dtype)] * 2
        remaining = [0, 1, 2]
        for axis in order:
            remaining.remove(axis)
            scratch.append(pltpu.VMEM((max(dims[axis] - 1, 1),) + tuple(dims[a] for a in remaining) + piece, grad.dtype))
    slots = 1 + sum(size - 1 for size in dims)
    outs = [jax.ShapeDtypeStruct(grad.shape[:-6] + grad.shape[-2:], jnp.float32) for grad in grads]
    return pl.pallas_call(
        functools.partial(scatter_kernel, dims, chunks, len(grads), orders),
        in_specs=[pl.BlockSpec(memory_space=pl.ANY)] * len(grads),
        out_specs=[pl.BlockSpec(memory_space=pltpu.VMEM)] * len(grads),
        out_shape=outs,
        scratch_shapes=scratch + [
            pltpu.SemaphoreType.DMA((len(chunks), slots)),
            pltpu.SemaphoreType.DMA((len(chunks), slots)),
            pltpu.SemaphoreType.DMA((len(chunks),)),
        ],
        compiler_params=pltpu.CompilerParams(collective_id=2, has_side_effects=True),
        name="scatter",
    )(*grads)


def adamw_step(master, gradient, first_moment, second_moment):
    first_new = beta_one * first_moment + (1.0 - beta_one) * gradient
    second_new = beta_two * second_moment + (1.0 - beta_two) * gradient * gradient
    fix_one = 1.0 - beta_one**STEP
    fix_two = 1.0 - beta_two**STEP
    update = -learn_rate * (
        first_new / fix_one / (jnp.sqrt(second_new / fix_two) + adam_eps) + weight_decay * master
    )
    return (update, first_new, second_new)


def per_device(
    tokens,
    cotangent,
    clip_start,
    clip_end,
    qkv_weight,
    out_weight,
    up_weight,
    down_weight,
    vectors,
    qkv_first,
    out_first,
    up_first,
    down_first,
    vector_first,
    qkv_second,
    out_second,
    up_second,
    down_second,
    vector_second,
):
    rows, width = tokens.shape
    device = lax.axis_index("dev")
    devices = lax.axis_size("dev")
    heads = width // HD
    reach = (rows + CLIP - 2) // rows
    base = reach * rows
    window_first = device * rows - base
    shards = (qkv_weight, out_weight, up_weight, down_weight, vectors)
    low = [shard.astype(jnp.bfloat16) for shard in shards]
    vector_part = jnp.pad(low[4].T, ((0, 0), (0, LANE - vectors.shape[0])))
    spans = jnp.pad(jnp.stack([clip_start, clip_end]), ((0, 6), (0, 0)))
    fulls, (tokens_window, spans_window) = gather(low[:1] + [vector_part] + low[1:4], [tokens, spans], devices)
    dims = chip_axes(devices)
    qkv_full = fulls[0].reshape(-1, width, width)
    vector_full = fulls[1].reshape(width, LANE)[:, : vectors.shape[0]].T.astype(jnp.float32)
    out_full = fulls[2].reshape(width, width)
    up_full = fulls[3].reshape(width, -1)
    down_full = fulls[4].reshape(-1, width)
    tokens_window = tokens_window.reshape(-1, width)
    spans_window = spans_window.transpose(1, 0, 2).reshape(8, -1)
    places = window_first + jnp.arange(spans_window.shape[1], dtype=jnp.int32)
    inside = (places >= 0) & (places < devices * rows)
    starts = jnp.where(inside, spans_window[0] - window_first, FAR)
    ends = jnp.where(inside, spans_window[1] - window_first, 0)
    own_start, own_end = clip_start - window_first, clip_end - window_first

    tq, tk = FORWARD_TILES
    forward_bounds = jnp.stack([own_start[::tq] // tk, (own_end[tq - 1 :: tq] + tk - 1) // tk], axis=1).reshape(-1)
    rq, rk = QUERY_TILES
    query_bounds = jnp.stack([own_start[::rq] // rk, (own_end[rq - 1 :: rq] + rk - 1) // rk], axis=1).reshape(-1)
    sk, sq = KEY_TILES
    last_keys = base + sk - 1 + jnp.arange(rows // sk, dtype=jnp.int32) * sk
    last_tiles = jnp.sum((starts[::sq][None, :] <= last_keys[:, None]).astype(jnp.int32), axis=1)
    first_tiles = own_start[::sk] // sq
    last_tiles = first_tiles + jnp.sum(((starts[::sq][None, :] <= last_keys[:, None]) & (jnp.arange(starts.shape[0] // sq)[None, :] >= first_tiles[:, None])).astype(jnp.int32), axis=1)
    key_bounds = jnp.stack([first_tiles, last_tiles], axis=1).reshape(-1)
    needed = jnp.stack([own_start[0] // PROJECT_TILE, (jnp.sum((inside & (starts < base + rows)).astype(jnp.int32)) + jnp.maximum(-window_first, 0) + PROJECT_TILE - 1) // PROJECT_TILE])

    query_window, key_window, value_window = project(tokens_window, vector_full, qkv_full, needed, PROJECT_TILE)
    own = lambda value: lax.slice_in_dim(value, base, base + rows, axis=0)
    query = own(query_window)
    lower, upper = own_start[:, None], own_end[:, None]
    mixed, lse = attend(query, key_window, value_window, lower, upper, forward_bounds, tq, tk, GROUP)
    up_bias = vector_full[8:].reshape(1, -1)
    (result, grad_middle, grad_mixed, delta, grad_out, grad_up, grad_down, middle_rows, bias_row) = middle_block(
        tokens, mixed, cotangent, vector_full, up_bias, out_full, up_full, down_full, MIDDLE_TILE, MIDDLE_CHUNK
    )
    table = jnp.concatenate([lse[:, :heads], delta[:, :heads]], axis=1).T
    grad_window, table_window = halo([grad_mixed, table], devices)
    grad_window = grad_window.reshape(-1, width)
    table_window = table_window.transpose(1, 0, 2).reshape(2 * heads, -1)
    groups = heads // (2 * GROUP)
    lse_window = table_window[:heads].reshape(groups, 2 * GROUP, -1)
    delta_window = table_window[heads:].reshape(groups, 2 * GROUP, -1)
    grad_query = query_grad(query, grad_mixed, key_window, value_window, lse, delta, lower, upper, query_bounds, rq, rk, GROUP)
    grad_keys, grad_values = key_grad(
        own(key_window), own(value_window), query_window, grad_window, lse_window, delta_window,
        starts[None, :], ends[None, :], key_bounds, base, sk, sq, GROUP,
    )
    grad_tokens, grad_qkv, last_rows = last_block(
        tokens, grad_middle, grad_query, grad_keys, grad_values, vector_full, qkv_full, LAST_TILE
    )
    grad_vectors = jnp.concatenate([last_rows[:4], middle_rows[:4], bias_row.reshape(-1, width)], axis=0)
    spread = lambda grad, lead=(): grad.reshape(lead + dims + (2, grad.shape[len(lead)] // devices, grad.shape[-1]))
    vector_rows = grad_vectors.reshape(vectors.shape[0], devices, -1).transpose(1, 0, 2).reshape(devices, -1)
    vector_rows = jnp.pad(vector_rows, ((0, 0), (0, 8 * LANE - vector_rows.shape[1]))).reshape(dims + (2, 8, LANE))
    owned = scatter([spread(grad_up), spread(grad_down), spread(grad_out), spread(grad_qkv, (3,)), vector_rows], devices)
    owned = (owned[3], owned[2], owned[0], owned[1], owned[4].reshape(-1)[: vectors.size].reshape(vectors.shape))
    firsts = (qkv_first, out_first, up_first, down_first, vector_first)
    seconds = (qkv_second, out_second, up_second, down_second, vector_second)
    stepped = [adamw_step(*four) for four in zip(shards, owned, firsts, seconds)]
    return (result, grad_tokens) + tuple(stepped[place][kind] for kind in range(3) for place in range(5))


def solution(mesh):
    in_specs = (
        P("dev", None),
        P("dev", None),
        P("dev"),
        P("dev"),
        P(None, "dev", None),
        P("dev", None),
        P("dev", None),
        P("dev", None),
        P(None, "dev"),
        P(None, "dev", None),
        P("dev", None),
        P("dev", None),
        P("dev", None),
        P(None, "dev"),
        P(None, "dev", None),
        P("dev", None),
        P("dev", None),
        P("dev", None),
        P(None, "dev"),
    )
    out_specs = (
        P("dev", None),
        P("dev", None),
        P(None, "dev", None),
        P("dev", None),
        P("dev", None),
        P("dev", None),
        P(None, "dev"),
        P(None, "dev", None),
        P("dev", None),
        P("dev", None),
        P("dev", None),
        P(None, "dev"),
        P(None, "dev", None),
        P("dev", None),
        P("dev", None),
        P("dev", None),
        P(None, "dev"),
    )
    return jax.shard_map(
        per_device, mesh=mesh, in_specs=in_specs, out_specs=out_specs, check_vma=False
    )
```

```python
import functools

import jax
import jax.numpy as jnp
from jax import lax
from jax.experimental import pallas as pl
from jax.experimental.pallas import tpu as pltpu
from jax.sharding import PartitionSpec as P

HD = 64
CLIP = 1500
STEP = 10
LANE = 128
FAR = 1 << 30
SQRT_HALF = 0.7071067811865476
INV_SQRT_TWO_PI = 0.3989422804014327


beta_one = 0.9
beta_two = 0.999
learn_rate = 0.02
weight_decay = 0.1
adam_eps = 1e-08
norm_eps = 1e-05
masked_score = -1e30
FORWARD_TILES = (256, 384)
QUERY_TILES = (256, 256)
KEY_TILES = (256, 256)
PROJECT_TILE = 768
MIDDLE_TILE = 256
MIDDLE_CHUNK = 512
LAST_TILE = 256
GROUP = 2
CHUNK_BYTES = 40000
PER_STEP = 4
HALO_START = 0
HALO_PASS = 3
GATHER_ORDERS = ((0, 1, 2), (0, 2, 1))
SCATTER_ORDERS = ((2, 1, 0), (1, 2, 0))
EXCHANGE_ORDERS = ((1, 2, 0), (1, 2, 0), (2, 1, 0))
SCATTER_PASS = 3
GATHER_LEVELS = (0, 1, 2, 3)
SCATTER_LEVELS = (0, 1, 2, 3, 4)
NT = (((1,), (1,)), ((), ()))
NN = (((1,), (0,)), ((), ()))


def shifted(value, axis, steps):
    count = lax.axis_size(axis)
    initial, last = (max(0, -steps), min(count, count - steps))
    return lax.ppermute(value, axis, [(source, source + steps) for source in range(initial, last)])


def dot(a, b, dims=NN):
    return lax.dot_general(a, b, dims, preferred_element_type=jnp.float32)


def stacked(pair, scale):
    lane = lax.broadcasted_iota(jnp.int32, pair.shape, 1)
    zero = jnp.zeros_like(pair)
    if scale is not None:
        pair = pair * jnp.asarray(scale, pair.dtype)
    return jnp.concatenate([jnp.where(lane < HD, pair, zero), jnp.where(lane >= HD, pair, zero)], axis=0)


def unstacked(both):
    rows = both.shape[0] // 2
    lane = lax.broadcasted_iota(jnp.int32, (rows, LANE), 1)
    return jnp.where(lane < HD, both[:rows], both[rows:])


def column(table, place):
    lane = lax.broadcasted_iota(jnp.int32, table.shape, 1)
    return jnp.sum(jnp.where(lane == place, table, 0.0), axis=1, keepdims=True)


def forward_kernel(tq, tk, pairs, bounds, lower, upper, q_ref, k_ref, v_ref, o_ref, lse_ref, qs, peak, acc):
    group = pl.program_id(0)
    tiles = q_ref.shape[0] // tq
    ones = jnp.ones((tk, LANE), jnp.bfloat16)

    @pl.when(group == 0)
    def _():
        lse_ref[...] = jnp.zeros_like(lse_ref)

    def one_tile(tile, none):
        rows = pl.ds(pl.multiple_of(tile * tq, tq), tq)
        for pair in range(pairs):
            qs[pair] = stacked(q_ref[rows, pair * LANE : (pair + 1) * LANE], HD ** -0.5)
        peak[...] = jnp.full_like(peak, masked_score)
        acc[...] = jnp.zeros_like(acc)
        low, high = lower[rows, :], upper[rows, :]

        def step(key_tile, none):
            first = pl.multiple_of(key_tile * tk, tk)
            places = first + lax.broadcasted_iota(jnp.int32, (tq, tk), 1)
            bias = jnp.where((places >= low) & (places < high), 0.0, masked_score)
            bias = jnp.concatenate([bias, bias], axis=0)
            for pair in range(pairs):
                lanes = slice(pair * LANE, (pair + 1) * LANE)
                scores = dot(qs[pair], k_ref[pl.ds(first, tk), lanes], NT) + bias
                old = peak[pair]
                new = jnp.maximum(old, jnp.max(scores, axis=1, keepdims=True))
                peak[pair] = new
                weights = jnp.exp(scores - jnp.concatenate([new] * (tk // LANE), axis=1)).astype(jnp.bfloat16)
                values = jnp.concatenate([v_ref[pl.ds(first, tk), lanes], ones], axis=1)
                scale = jnp.exp(old - new)
                acc[pair] = acc[pair] * jnp.concatenate([scale, scale], axis=1) + dot(weights, values)
            return none

        lax.fori_loop(bounds[2 * tile], bounds[2 * tile + 1], step, 0)
        lane = lax.broadcasted_iota(jnp.int32, (tq, LANE), 1)
        table = lse_ref[rows, :]
        for pair in range(pairs):
            both = acc[pair]
            total = both[:, LANE:]
            o_ref[rows, pair * LANE : (pair + 1) * LANE] = unstacked(both[:, :LANE] / total).astype(o_ref.dtype)
            logs = peak[pair] + jnp.log(total)
            head = (group * pairs + pair) * 2
            table = jnp.where(lane == head, logs[:tq], table)
            table = jnp.where(lane == head + 1, logs[tq:], table)
        lse_ref[rows, :] = table
        return none

    lax.fori_loop(0, tiles, one_tile, 0)


def attend(query, keys, values, lower, upper, bounds, tq, tk, pairs):
    rows, (window, width) = lower.shape[0], keys.shape
    middle = window // rows // 2
    lanes = pairs * LANE
    return pl.pallas_call(
        functools.partial(forward_kernel, tq, tk, pairs),
        grid_spec=pltpu.PrefetchScalarGridSpec(
            num_scalar_prefetch=1, grid=(width // lanes,),
            in_specs=[
                pl.BlockSpec((rows, 1), lambda g, b: (0, 0)),
                pl.BlockSpec((rows, 1), lambda g, b: (0, 0)),
                pl.BlockSpec((rows, lanes), lambda g, b: (middle, g)),
                pl.BlockSpec((window, lanes), lambda g, b: (0, g)),
                pl.BlockSpec((window, lanes), lambda g, b: (0, g)),
            ],
            out_specs=[pl.BlockSpec((rows, lanes), lambda g, b: (0, g)), pl.BlockSpec((rows, LANE), lambda g, b: (0, 0))],
            scratch_shapes=[
                pltpu.VMEM((pairs, 2 * tq, LANE), jnp.bfloat16),
                pltpu.VMEM((pairs, 2 * tq, LANE), jnp.float32),
                pltpu.VMEM((pairs, 2 * tq, 2 * LANE), jnp.float32),
            ],
        ),
        out_shape=[jax.ShapeDtypeStruct((rows, width), jnp.bfloat16), jax.ShapeDtypeStruct((rows, LANE), jnp.float32)],
        name="attend",
    )(bounds, lower, upper, query, keys, values)


def query_grad_kernel(tq, tk, pairs, bounds, lower, upper, q_ref, g_ref, k_ref, v_ref, lse_ref, delta_ref, dq_ref, qs, gs, logs, deltas, acc):
    group = pl.program_id(0)
    tiles = q_ref.shape[0] // tq

    def one_tile(tile, none):
        rows = pl.ds(pl.multiple_of(tile * tq, tq), tq)
        table, other = lse_ref[rows, :], delta_ref[rows, :]
        for pair in range(pairs):
            lanes = slice(pair * LANE, (pair + 1) * LANE)
            qs[pair] = stacked(q_ref[rows, lanes], HD ** -0.5)
            gs[pair] = stacked(g_ref[rows, lanes], None)
            head = (group * pairs + pair) * 2
            logs[pair] = jnp.broadcast_to(jnp.concatenate([column(table, head), column(table, head + 1)], axis=0), logs.shape[1:])
            deltas[pair] = jnp.broadcast_to(jnp.concatenate([column(other, head), column(other, head + 1)], axis=0), logs.shape[1:])
        acc[...] = jnp.zeros_like(acc)
        low, high = lower[rows, :], upper[rows, :]

        def step(key_tile, none):
            first = pl.multiple_of(key_tile * tk, tk)
            places = first + lax.broadcasted_iota(jnp.int32, (tq, tk), 1)
            bias = jnp.where((places >= low) & (places < high), 0.0, masked_score)
            bias = jnp.concatenate([bias, bias], axis=0)
            for pair in range(pairs):
                lanes = slice(pair * LANE, (pair + 1) * LANE)
                keys = k_ref[pl.ds(first, tk), lanes]
                scores = dot(qs[pair], keys, NT) + bias
                probs = jnp.exp(scores - jnp.concatenate([logs[pair]] * (tk // LANE), axis=1))
                grad_probs = dot(gs[pair], v_ref[pl.ds(first, tk), lanes], NT)
                grad_scores = (probs * (grad_probs - jnp.concatenate([deltas[pair]] * (tk // LANE), axis=1))).astype(jnp.bfloat16)
                acc[pair] += dot(grad_scores, keys)
            return none

        lax.fori_loop(bounds[2 * tile], bounds[2 * tile + 1], step, 0)
        for pair in range(pairs):
            dq_ref[rows, pair * LANE : (pair + 1) * LANE] = (unstacked(acc[pair]) * HD ** -0.5).astype(dq_ref.dtype)
        return none

    lax.fori_loop(0, tiles, one_tile, 0)


def query_grad(query, grad, keys, values, lse, delta, lower, upper, bounds, tq, tk, pairs):
    (rows, width), window = grad.shape, keys.shape[0]
    middle = window // rows // 2
    lanes = pairs * LANE
    own = lambda at=0: pl.BlockSpec((rows, lanes), lambda g, b: (at, g))
    far = lambda: pl.BlockSpec((window, lanes), lambda g, b: (0, g))
    fixed = lambda cols: pl.BlockSpec((rows, cols), lambda g, b: (0, 0))
    return pl.pallas_call(
        functools.partial(query_grad_kernel, tq, tk, pairs),
        grid_spec=pltpu.PrefetchScalarGridSpec(
            num_scalar_prefetch=1, grid=(width // lanes,),
            in_specs=[fixed(1), fixed(1), own(middle), own(), far(), far(), fixed(LANE), fixed(LANE)],
            out_specs=own(),
            scratch_shapes=[
                pltpu.VMEM((pairs, 2 * tq, LANE), jnp.bfloat16),
                pltpu.VMEM((pairs, 2 * tq, LANE), jnp.bfloat16),
                pltpu.VMEM((pairs, 2 * tq, LANE), jnp.float32),
                pltpu.VMEM((pairs, 2 * tq, LANE), jnp.float32),
                pltpu.VMEM((pairs, 2 * tq, LANE), jnp.float32),
            ],
        ),
        out_shape=jax.ShapeDtypeStruct((rows, width), jnp.bfloat16),
        name="query_grad",
    )(bounds, lower, upper, query, grad, keys, values, lse, delta)


def key_grad_kernel(tk, tq, pairs, base, bounds, lower, upper, k_ref, v_ref, q_ref, g_ref, lse_ref, delta_ref, dk_ref, dv_ref, ks, vs, acc):
    tiles = k_ref.shape[0] // tk

    def one_tile(tile, none):
        rows = pl.ds(pl.multiple_of(tile * tk, tk), tk)
        for pair in range(pairs):
            lanes = slice(pair * LANE, (pair + 1) * LANE)
            ks[pair] = stacked(k_ref[rows, lanes], HD ** -0.5)
            vs[pair] = stacked(v_ref[rows, lanes], None)
        acc[...] = jnp.zeros_like(acc)

        def step(query_tile, none):
            first = pl.multiple_of(query_tile * tq, tq)
            here = pl.ds(first, tq)
            places = base + tile * tk + lax.broadcasted_iota(jnp.int32, (tk, tq), 0)
            bias = jnp.where((places >= lower[:, here]) & (places < upper[:, here]), 0.0, masked_score)
            for pair in range(pairs):
                lanes = slice(pair * LANE, (pair + 1) * LANE)
                queries, grads = q_ref[here, lanes], g_ref[here, lanes]
                scores = dot(ks[pair], queries, NT)
                grad_probs = dot(vs[pair], grads, NT)
                probs, grad_scores = [], []
                for half in range(2):
                    part = slice(half * tk, (half + 1) * tk)
                    head = slice(2 * pair + half, 2 * pair + half + 1)
                    prob = jnp.exp(scores[part] + bias - lse_ref[0, head, here])
                    probs.append(prob.astype(jnp.bfloat16))
                    grad_scores.append((prob * (grad_probs[part] - delta_ref[0, head, here])).astype(jnp.bfloat16))
                acc[pair, :, :LANE] += dot(jnp.concatenate(grad_scores, axis=0), queries)
                acc[pair, :, LANE:] += dot(jnp.concatenate(probs, axis=0), grads)
            return none

        lax.fori_loop(bounds[2 * tile], bounds[2 * tile + 1], step, 0)
        for pair in range(pairs):
            lanes = slice(pair * LANE, (pair + 1) * LANE)
            dk_ref[rows, lanes] = (unstacked(acc[pair, :, :LANE]) * HD ** -0.5).astype(dk_ref.dtype)
            dv_ref[rows, lanes] = unstacked(acc[pair, :, LANE:]).astype(dv_ref.dtype)
        return none

    lax.fori_loop(0, tiles, one_tile, 0)


def key_grad(keys, values, query, grad, lse, delta, lower, upper, bounds, base, rows, tk, tq, pairs):
    window, width = query.shape
    middle = base // rows
    lanes = pairs * LANE
    own = lambda at=0: pl.BlockSpec((rows, lanes), lambda g, b: (at, g))
    far = lambda: pl.BlockSpec((window, lanes), lambda g, b: (0, g))
    line = lambda: pl.BlockSpec((1, window), lambda g, b: (0, 0))
    heads = lambda: pl.BlockSpec((1, 2 * pairs, window), lambda g, b: (g, 0, 0))
    return pl.pallas_call(
        functools.partial(key_grad_kernel, tk, tq, pairs, base),
        grid_spec=pltpu.PrefetchScalarGridSpec(
            num_scalar_prefetch=1, grid=(width // lanes,),
            in_specs=[line(), line(), own(middle), own(middle), far(), far(), heads(), heads()],
            out_specs=[own(), own()],
            scratch_shapes=[
                pltpu.VMEM((pairs, 2 * tk, LANE), jnp.bfloat16),
                pltpu.VMEM((pairs, 2 * tk, LANE), jnp.bfloat16),
                pltpu.VMEM((pairs, 2 * tk, 2 * LANE), jnp.float32),
            ],
        ),
        out_shape=[jax.ShapeDtypeStruct((rows, width), jnp.bfloat16)] * 2,
        name="key_grad",
    )(bounds, lower, upper, keys, values, query, grad, lse, delta)


def units(values):
    centre = values - jnp.mean(values, axis=-1, keepdims=True)
    inverse = lax.rsqrt(jnp.mean(centre * centre, axis=-1, keepdims=True) + norm_eps)
    return centre * inverse, inverse


def norm_pull(grad_output, unit, inverse, gain):
    grad_unit = grad_output * gain
    first = jnp.mean(grad_unit, axis=-1, keepdims=True)
    second = jnp.mean(grad_unit * unit, axis=-1, keepdims=True)
    return inverse * (grad_unit - first - unit * second)


def row_sum(values):
    return jnp.sum(values, axis=0, keepdims=True)


def gelu_pair(hidden):
    inner = 0.5 + 0.5 * lax.erf(hidden * SQRT_HALF)
    slope = inner + hidden * (jnp.exp(-0.5 * hidden * hidden) * INV_SQRT_TWO_PI)
    return hidden * inner, slope


def project_kernel(tile, active, tokens, vectors, weights, query, keys, values):
    place = pl.program_id(0)
    needed = (place >= active[0]) & (place < active[1])

    @pl.when(needed)
    def _():
        unit = units(tokens[...].astype(jnp.float32))[0]
        normed = (unit * vectors[0:1, :] + vectors[1:2, :]).astype(jnp.bfloat16)
        query[...] = (dot(normed, weights[0]) + vectors[2:3, :]).astype(query.dtype)
        keys[...] = dot(normed, weights[1]).astype(keys.dtype)
        values[...] = (dot(normed, weights[2]) + vectors[3:4, :]).astype(values.dtype)

    @pl.when(jnp.logical_not(needed))
    def _():
        for out in (query, keys, values):
            out[...] = jnp.zeros_like(out)


def project(tokens, vectors, weights, active, tile):
    rows, width = tokens.shape
    block = lambda: pl.BlockSpec((tile, width), lambda i, b: (i, 0))
    return pl.pallas_call(
        functools.partial(project_kernel, tile),
        grid_spec=pltpu.PrefetchScalarGridSpec(
            num_scalar_prefetch=1, grid=(rows // tile,),
            in_specs=[
                block(),
                pl.BlockSpec(vectors.shape, lambda i, b: (0, 0)),
                pl.BlockSpec(weights.shape, lambda i, b: (0, 0, 0)),
            ],
            out_specs=[block(), block(), block()],
        ),
        out_shape=[jax.ShapeDtypeStruct((rows, width), jnp.bfloat16)] * 3,
        name="project",
    )(active, tokens, vectors, weights)


def middle_kernel(tile, tokens, mixed, cotangent, vectors, up_bias, out_weight, up_weight, down_weight,
                  result, grad_middle, grad_mixed, delta, grad_out, grad_up, grad_down, grad_rows, grad_bias,
                  middle, normed, turned, total, back, actives, hiddens):
    place, count = pl.program_id(0), pl.num_programs(0)
    rows = tokens.shape[0]
    parts = [slice(i, i + tile) for i in range(0, rows, tile)]

    @pl.when(place == 0)
    def _():
        for part in parts:
            branch = dot(mixed[part, :], out_weight[...]) + vectors[4:5, :]
            wide = tokens[part, :].astype(jnp.float32) + branch
            middle[part, :] = wide
            unit = units(wide)[0]
            low = (unit * vectors[5:6, :] + vectors[6:7, :]).astype(jnp.bfloat16)
            normed[part, :] = low
            turned[:, part] = low.T
            total[part, :] = wide + vectors[7:8, :]
        back[...] = jnp.zeros_like(back)

    bias = jnp.zeros_like(grad_bias)
    for part in parts:
        hidden = dot(normed[part, :], up_weight[...]) + up_bias[...]
        wide, slope = gelu_pair(hidden)
        active = wide.astype(jnp.bfloat16)
        grad_active = dot(cotangent[part, :], down_weight[...], NT)
        grad_hidden = (grad_active * slope).astype(jnp.bfloat16)
        actives[part, :] = active
        hiddens[part, :] = grad_hidden
        bias += row_sum(grad_hidden.astype(jnp.float32))
        total[part, :] += dot(active, down_weight[...])
        back[part, :] += dot(grad_hidden, up_weight[...], NT)
    grad_bias[...] = bias
    grad_up[...] = dot(turned[...], hiddens[...]).astype(grad_up.dtype)
    grad_down[...] = dot(actives[...], cotangent[...], (((0,), (0,)), ((), ()))).astype(grad_down.dtype)

    @pl.when(place == count - 1)
    def _():
        sums = [jnp.zeros((1, tokens.shape[1]), jnp.float32) for _ in range(4)]
        for part in parts:
            result[part, :] = total[part, :].astype(result.dtype)
            unit, inverse = units(middle[part, :])
            incoming = back[part, :]
            wide = cotangent[part, :].astype(jnp.float32)
            grad = wide + norm_pull(incoming, unit, inverse, vectors[5:6, :])
            grad_middle[part, :] = grad
            branch = grad.astype(jnp.bfloat16)
            turned[:, part] = mixed[part, :].T
            hiddens_low = dot(branch, out_weight[...], NT).astype(jnp.bfloat16)
            grad_mixed[part, :] = hiddens_low
            product = hiddens_low.astype(jnp.float32) * mixed[part, :].astype(jnp.float32)
            delta[part, :] = head_sums(product)
            normed[part, :] = branch
            sums[0] += row_sum(branch.astype(jnp.float32))
            sums[1] += row_sum(incoming * unit)
            sums[2] += row_sum(incoming)
            sums[3] += row_sum(wide)
        grad_out[...] = dot(turned[...], normed[...]).astype(grad_out.dtype)
        grad_rows[...] = jnp.concatenate(sums + [jnp.zeros((4, tokens.shape[1]), jnp.float32)], axis=0)


def head_sums(product):
    rows, width = product.shape
    lane = lax.broadcasted_iota(jnp.int32, (rows, LANE), 1)
    table = jnp.zeros((rows, LANE), jnp.float32)
    for pair in range(width // LANE):
        piece = product[:, pair * LANE : (pair + 1) * LANE]
        first = jnp.sum(jnp.where(lane < HD, piece, 0.0), axis=1, keepdims=True)
        second = jnp.sum(jnp.where(lane >= HD, piece, 0.0), axis=1, keepdims=True)
        table = jnp.where(lane == 2 * pair, first, table)
        table = jnp.where(lane == 2 * pair + 1, second, table)
    return table


def middle_block(tokens, mixed, cotangent, vectors, up_bias, out_weight, up_weight, down_weight, tile, chunk):
    rows, width = tokens.shape
    hidden = up_weight.shape[1]
    whole = lambda shape: pl.BlockSpec(shape, lambda i: (0,) * len(shape))
    across = lambda r: pl.BlockSpec((r, chunk), lambda i: (0, i))
    down = lambda: pl.BlockSpec((chunk, width), lambda i: (i, 0))
    full = (rows, width)
    return pl.pallas_call(
        functools.partial(middle_kernel, tile),
        grid=(hidden // chunk,),
        in_specs=[whole(full), whole(full), whole(full), whole(vectors.shape), across(1), whole((width, width)), across(width), down()],
        out_specs=[whole(full), whole(full), whole(full), whole((rows, LANE)), whole((width, width)), across(width), down(), whole((8, width)), across(1)],
        out_shape=[
            jax.ShapeDtypeStruct(full, jnp.bfloat16),
            jax.ShapeDtypeStruct(full, jnp.float32),
            jax.ShapeDtypeStruct(full, jnp.bfloat16),
            jax.ShapeDtypeStruct((rows, LANE), jnp.float32),
            jax.ShapeDtypeStruct((width, width), jnp.bfloat16),
            jax.ShapeDtypeStruct((width, hidden), jnp.bfloat16),
            jax.ShapeDtypeStruct((hidden, width), jnp.bfloat16),
            jax.ShapeDtypeStruct((8, width), jnp.float32),
            jax.ShapeDtypeStruct((1, hidden), jnp.float32),
        ],
        scratch_shapes=[
            pltpu.VMEM(full, jnp.float32),
            pltpu.VMEM(full, jnp.bfloat16),
            pltpu.VMEM((width, rows), jnp.bfloat16),
            pltpu.VMEM(full, jnp.float32),
            pltpu.VMEM(full, jnp.float32),
            pltpu.VMEM((rows, chunk), jnp.bfloat16),
            pltpu.VMEM((rows, chunk), jnp.bfloat16),
        ],
        name="middle",
    )(tokens, mixed, cotangent, vectors, up_bias, out_weight, up_weight, down_weight)


def last_kernel(tile, tokens, grad_middle, grad_query, grad_keys, grad_values, vectors, weights,
                grad_tokens, grad_qkv, grad_rows, turned):
    rows, width = tokens.shape
    sums = [jnp.zeros((1, width), jnp.float32) for _ in range(4)]
    for first in range(0, rows, tile):
        part = slice(first, first + tile)
        unit, inverse = units(tokens[part, :].astype(jnp.float32))
        turned[:, part] = (unit * vectors[0:1, :] + vectors[1:2, :]).astype(jnp.bfloat16).T
        incoming = dot(grad_query[part, :], weights[0], NT)
        incoming += dot(grad_keys[part, :], weights[1], NT)
        incoming += dot(grad_values[part, :], weights[2], NT)
        grad_tokens[part, :] = grad_middle[part, :] + norm_pull(incoming, unit, inverse, vectors[0:1, :])
        sums[0] += row_sum(incoming * unit)
        sums[1] += row_sum(incoming)
        sums[2] += row_sum(grad_query[part, :].astype(jnp.float32))
        sums[3] += row_sum(grad_values[part, :].astype(jnp.float32))
    for place, grad in enumerate((grad_query, grad_keys, grad_values)):
        grad_qkv[place] = dot(turned[...], grad[...]).astype(grad_qkv.dtype)
    grad_rows[...] = jnp.concatenate(sums + [jnp.zeros((4, width), jnp.float32)], axis=0)


def last_block(tokens, grad_middle, grad_query, grad_keys, grad_values, vectors, weights, tile):
    rows, width = tokens.shape
    return pl.pallas_call(
        functools.partial(last_kernel, tile),
        out_shape=[
            jax.ShapeDtypeStruct((rows, width), jnp.float32),
            jax.ShapeDtypeStruct(weights.shape, jnp.bfloat16),
            jax.ShapeDtypeStruct((8, width), jnp.float32),
        ],
        scratch_shapes=[pltpu.VMEM((width, rows), jnp.bfloat16)],
        name="last",
    )(tokens, grad_middle, grad_query, grad_keys, grad_values, vectors, weights)


def chip_axes(devices):
    chips = devices // 2
    return {16: (4, 2, 2), 64: (4, 4, 4)}.get(chips, (chips, 1, 1))


class Place:
    def __init__(self, dims):
        self.dims = dims
        self.me = lax.axis_index("dev")
        self.core = lax.rem(self.me, 2)
        chip = self.me // 2
        self.at = (chip // (dims[1] * dims[2]), lax.rem(chip // dims[2], dims[1]), lax.rem(chip, dims[2]))
        self.partner = self.me + 1 - 2 * self.core

    def peer(self, axis, step):
        there = lax.rem(self.at[axis] + step, self.dims[axis])
        at = [there if a == axis else self.at[a] for a in range(3)]
        return ((at[0] * self.dims[1] + at[1]) * self.dims[2] + at[2]) * 2 + self.core, there

    def peers(self):
        return [self.partner] + [self.peer(axis, step)[0] for axis in range(3) for step in range(1, self.dims[axis])]


def remote(source, target, send, recv, device):
    return pltpu.make_async_remote_copy(
        src_ref=source, dst_ref=target, send_sem=send, recv_sem=recv,
        device_id=(device,), device_id_type=pl.DeviceIdType.MESH,
    )


def greet(peers, around=None, devices=0):
    barrier = pltpu.get_barrier_semaphore()
    count = len(peers)
    for peer in peers:
        pl.semaphore_signal(barrier, inc=1, device_id=(peer,), device_id_type=pl.DeviceIdType.MESH)
    if around is not None:
        for other in (around - 2, around + 2):
            there = (other >= 0) & (other < devices)
            count = count + there.astype(jnp.int32)

            @pl.when(there)
            def _():
                pl.semaphore_signal(barrier, inc=1, device_id=(other,), device_id_type=pl.DeviceIdType.MESH)

    pl.semaphore_wait(barrier, count)


class Halo:
    def __init__(self, place, devices, own, window, send, recv, local):
        self.place, self.devices, self.own, self.window = place, devices, own, window
        self.send, self.recv, self.local = send, recv, local
        me, core = place.me, place.core
        self.above, self.below = me + 2 < devices, me >= 2
        self.up = remote(own, window.at[0], send.at[0], recv.at[0], me + 2)
        self.down = remote(own, window.at[4], send.at[1], recv.at[1], me - 2)
        side = jnp.where(core == 0, 1, 3)
        self.across = remote(own, window.at[side], send.at[2], recv.at[2], place.partner)
        self.kept = jnp.where(core == 0, 4, 0)
        self.relay = remote(window.at[self.kept], window.at[4 - side], send.at[3], recv.at[3], place.partner)
        self.keep = pltpu.make_async_copy(own, window.at[2], local)

    def start(self):
        pl.when(self.above)(self.up.start)
        pl.when(self.below)(self.down.start)
        self.across.start()
        self.keep.start()

    def pass_on(self):
        pl.when(self.below)(self.up.wait_recv)
        pl.when(self.above)(self.down.wait_recv)
        even = self.place.core == 0
        self.relays = jnp.where(even, self.above, self.below)
        pl.when(self.relays)(self.relay.start)

    def finish(self):
        even = self.place.core == 0
        comes = jnp.where(even, self.below, self.above)
        self.across.wait_recv()
        pl.when(comes)(self.relay.wait_recv)
        self.keep.wait()
        pl.when(self.above)(self.up.wait_send)
        pl.when(self.below)(self.down.wait_send)
        self.across.wait_send()
        pl.when(self.relays)(self.relay.wait_send)


def gather_kernel(dims, devices, chunks, orders, arrays, halos, *refs):
    shards, owns = refs[:arrays], refs[arrays : arrays + halos]
    fulls = refs[arrays + halos : 2 * arrays + halos]
    windows = refs[2 * arrays + halos : 2 * (arrays + halos)]
    scratch = refs[2 * (arrays + halos) :]
    wides, shards = shards, scratch[:arrays]
    send, recv, local, halo_send, halo_recv, halo_local = scratch[arrays:]
    place = Place(dims)
    for wide, shard in zip(wides, shards):
        shard[...] = wide[...].astype(shard.dtype)
    greet(place.peers(), place.me, devices)
    parts = [
        Halo(place, devices, owns[i], windows[i], halo_send.at[i], halo_recv.at[i], halo_local.at[i])
        for i in range(halos)
    ]
    count = len(chunks)
    started = {}

    def stage(number, level):
        array, lead, lanes = chunks[number]
        shard, full = shards[array], fulls[array]
        front = () if lead is None else (lead,)
        source = shard.at[front + (slice(None), lanes)] if front else shard.at[:, lanes]
        order = orders[number]
        done = order[: min(level, 3)]
        index = tuple(slice(None) if axis in done else place.at[axis] for axis in range(3))
        view = lambda index, core: full.at[front + index + (core, slice(None), lanes)]
        if level == 0:
            mine = pltpu.make_async_copy(source, view(index, place.core), local.at[number])
            mine.start()
            started[number] = [mine]
        else:
            for copy in started[number, level - 1]:
                copy.wait_recv()
            if level == 1:
                started[number][0].wait()
            source = view(index, place.core)
        copies = []
        if level == 3:
            copies.append(remote(source, source, send.at[number, 0], recv.at[number, 0], place.partner))
        else:
            base = 1 + sum(dims[axis] - 1 for axis in order[:level])
            for step in range(1, dims[order[level]]):
                slot = base + step - 1
                device = place.peer(order[level], step)[0]
                target = view(index, place.core)
                copies.append(remote(source, target, send.at[number, slot], recv.at[number, slot], device))
        for copy in copies:
            copy.start()
        started[number, level] = copies

    steps = -(-count // PER_STEP)
    for time in range(steps + 3):
        for level in GATHER_LEVELS:
            for number in range((time - level) * PER_STEP, (time - level + 1) * PER_STEP):
                if 0 <= number < count:
                    stage(number, level)
        if time == HALO_START:
            for part in parts:
                part.start()
        if time == min(HALO_PASS, steps + 2):
            for part in parts:
                part.pass_on()
    for number in range(count):
        for copy in started[number, 3]:
            copy.wait_recv()
        for level in range(4):
            for copy in started[number, level]:
                copy.wait_send()
    for part in parts:
        part.finish()


def gather(shards, owns, devices):
    dims = chip_axes(devices)
    chunks = []
    for array, shard in enumerate(shards):
        lanes = shard.shape[-1]
        if shard.ndim == 3:
            chunks += [(array, lead, slice(0, lanes)) for lead in range(shard.shape[0])]
        else:
            wide = min(lanes, max(CHUNK_BYTES // (2 * shard.shape[0]) // LANE * LANE, LANE))
            wide = max(w for w in range(LANE, wide + 1, LANE) if lanes % w == 0)
            chunks += [(array, None, slice(first, first + wide)) for first in range(0, lanes, wide)]
    orders = [GATHER_ORDERS[number % len(GATHER_ORDERS)] for number in range(len(chunks))]
    slots = 1 + sum(size - 1 for size in dims)
    anywhere = pl.BlockSpec(memory_space=pl.ANY)
    inside = pl.BlockSpec(memory_space=pltpu.VMEM)
    outs = [
        jax.ShapeDtypeStruct(shard.shape[:-2] + dims + (2,) + shard.shape[-2:], jnp.bfloat16) for shard in shards
    ] + [jax.ShapeDtypeStruct((5,) + own.shape, own.dtype) for own in owns]
    done = pl.pallas_call(
        functools.partial(gather_kernel, dims, devices, chunks, orders, len(shards), len(owns)),
        in_specs=[inside] * (len(shards) + len(owns)),
        out_specs=[anywhere] * len(outs),
        out_shape=outs,
        scratch_shapes=[pltpu.VMEM(shard.shape, jnp.bfloat16) for shard in shards] + [
            pltpu.SemaphoreType.DMA((len(chunks), slots)),
            pltpu.SemaphoreType.DMA((len(chunks), slots)),
            pltpu.SemaphoreType.DMA((len(chunks),)),
            pltpu.SemaphoreType.DMA((max(len(owns), 1), 4)),
            pltpu.SemaphoreType.DMA((max(len(owns), 1), 4)),
            pltpu.SemaphoreType.DMA((max(len(owns), 1),)),
        ],
        compiler_params=pltpu.CompilerParams(collective_id=0, has_side_effects=True),
        name="gather",
    )(*shards, *owns)
    return done[: len(shards)], done[len(shards) :]


def scatter_kernel(dims, devices, chunks, arrays, halos, orders, *refs):
    grads, owns = refs[:arrays], refs[arrays : arrays + halos]
    outs = refs[arrays + halos : 2 * arrays + halos]
    windows = refs[2 * arrays + halos : 2 * (arrays + halos)]
    rest = refs[2 * (arrays + halos) :]
    count = len(chunks)
    buffers = [rest[5 * i : 5 * i + 5] for i in range(count)]
    send, recv, local, halo_send, halo_recv, halo_local = rest[5 * count :]
    place = Place(dims)
    if halos:
        greet(place.peers(), place.me, devices)
    else:
        greet(place.peers())
    parts = [
        Halo(place, devices, owns[i], windows[i], halo_send.at[i], halo_recv.at[i], halo_local.at[i])
        for i in range(halos)
    ]
    for part in parts:
        part.start()
    started = {}

    def source(number, core):
        array, lead, lanes = chunks[number]
        front = () if lead is None else (lead,)
        return grads[array].at[front + (slice(None), slice(None), slice(None), core, slice(None), lanes)]

    def spread(shape, one):
        total = 1
        for size in shape:
            total *= size

        def body(flat, none):
            index = []
            for size in reversed(shape):
                index.insert(0, lax.rem(flat, size))
                flat = flat // size
            one(tuple(index))
            return none

        lax.fori_loop(0, total, body, 0)

    def stage(number, level):
        own, first, second, third, fourth = buffers[number]
        order = orders[number]
        held = (own, second, third, fourth)
        copies = []
        if level == 0:
            mine = pltpu.make_async_copy(source(number, place.core), own, local.at[number])
            mine.start()
            started[number] = mine
            copies.append(remote(source(number, 1 - place.core), first, send.at[number, 0], recv.at[number, 0], place.partner))
        else:
            for copy in started[number, level - 1]:
                copy.wait_recv()
            remaining = [axis for axis in range(3) if axis not in order[: level - 1]]
            if level == 1:
                started[number].wait()

                def add(index):
                    total = own[index].astype(jnp.float32) + first[index].astype(jnp.float32)
                    own[index] = total.astype(own.dtype)

                spread(dims, add)
            else:
                combine(number, level)
            axis = order[level - 1]
            base = 1 + sum(dims[a] - 1 for a in order[: level - 1])
            for step in range(1, dims[axis]):
                device, there = place.peer(axis, step)
                where = tuple(there if a == axis else slice(None) for a in remaining)
                slot = base + step - 1
                piece = (own if level == 1 else held[level - 1].at[0]).at[where]
                copies.append(remote(piece, held[level].at[step - 1], send.at[number, slot], recv.at[number, slot], device))
        for copy in copies:
            copy.start()
        started[number, level] = copies

    def combine(number, level):
        own, first, second, third, fourth = buffers[number]
        order = orders[number]
        held = (own, second, third, fourth)
        axis = order[level - 2]
        before = [a for a in range(3) if a not in order[: level - 2]]
        after = [a for a in before if a != axis]
        slots = dims[axis] - 1
        old = own if level == 2 else held[level - 2].at[0]
        new = held[level - 1]
        array, lead, lanes = chunks[number]

        def add(index):
            where = list(index)
            where.insert(before.index(axis), place.at[axis])
            total = old[tuple(where)].astype(jnp.float32)
            for slot in range(slots):
                total += new[(slot,) + index].astype(jnp.float32)
            if level == 4:
                if lead is None:
                    outs[array][:, lanes] = total
                else:
                    outs[array][lead, :, lanes] = total
            else:
                new[(0,) + index] = total.astype(new.dtype)

        if after:
            spread([dims[a] for a in after], add)
        else:
            add(())

    steps = -(-count // PER_STEP)
    for time in range(steps + 4):
        if time == min(SCATTER_PASS, steps + 3):
            for part in parts:
                part.pass_on()
        for level in SCATTER_LEVELS:
            for number in range((time - level) * PER_STEP, (time - level + 1) * PER_STEP):
                if not 0 <= number < count:
                    continue
                if level == 4:
                    for copy in started[number, 3]:
                        copy.wait_recv()
                    combine(number, 4)
                else:
                    stage(number, level)
    for number in range(count):
        for level in range(4):
            for copy in started[number, level]:
                copy.wait_send()
    for part in parts:
        part.finish()


def scatter(grads, owns, devices, orders, identity):
    dims = chip_axes(devices)
    chunks = []
    for array, grad in enumerate(grads):
        rows, lanes = grad.shape[-2:]
        if grad.ndim == 7:
            chunks += [(array, lead, slice(0, lanes)) for lead in range(grad.shape[0])]
        else:
            wide = min(lanes, max(CHUNK_BYTES // (2 * rows) // LANE * LANE, LANE))
            wide = max(w for w in range(LANE, wide + 1, LANE) if lanes % w == 0)
            chunks += [(array, None, slice(first, first + wide)) for first in range(0, lanes, wide)]
    orders = [orders[number % len(orders)] for number in range(len(chunks))]
    scratch = []
    for (array, lead, lanes), order in zip(chunks, orders):
        grad = grads[array]
        piece = (grad.shape[-2], lanes.stop - lanes.start)
        left = [dims[a] for a in range(3)]
        scratch += [pltpu.VMEM(dims + piece, grad.dtype)] * 2
        remaining = [0, 1, 2]
        for axis in order:
            remaining.remove(axis)
            scratch.append(pltpu.VMEM((max(dims[axis] - 1, 1),) + tuple(dims[a] for a in remaining) + piece, grad.dtype))
    slots = 1 + sum(size - 1 for size in dims)
    outs = [jax.ShapeDtypeStruct(grad.shape[:-6] + grad.shape[-2:], jnp.float32) for grad in grads]
    outs += [jax.ShapeDtypeStruct((5,) + own.shape, own.dtype) for own in owns]
    anywhere = pl.BlockSpec(memory_space=pl.ANY)
    inside = pl.BlockSpec(memory_space=pltpu.VMEM)
    done = pl.pallas_call(
        functools.partial(scatter_kernel, dims, devices, chunks, len(grads), len(owns), orders),
        in_specs=[anywhere] * len(grads) + [inside] * len(owns),
        out_specs=[inside] * len(grads) + [anywhere] * len(owns),
        out_shape=outs,
        scratch_shapes=scratch + [
            pltpu.SemaphoreType.DMA((len(chunks), slots)),
            pltpu.SemaphoreType.DMA((len(chunks), slots)),
            pltpu.SemaphoreType.DMA((len(chunks),)),
            pltpu.SemaphoreType.DMA((max(len(owns), 1), 4)),
            pltpu.SemaphoreType.DMA((max(len(owns), 1), 4)),
            pltpu.SemaphoreType.DMA((max(len(owns), 1),)),
        ],
        compiler_params=pltpu.CompilerParams(collective_id=identity, has_side_effects=True),
        name="scatter" if not owns else "exchange",
    )(*grads, *owns)
    return done[: len(grads)], done[len(grads) :]


def adamw_step(master, gradient, first_moment, second_moment):
    first_new = beta_one * first_moment + (1.0 - beta_one) * gradient
    second_new = beta_two * second_moment + (1.0 - beta_two) * gradient * gradient
    fix_one = 1.0 - beta_one**STEP
    fix_two = 1.0 - beta_two**STEP
    update = -learn_rate * (
        first_new / fix_one / (jnp.sqrt(second_new / fix_two) + adam_eps) + weight_decay * master
    )
    return (update, first_new, second_new)


def per_device(
    tokens,
    cotangent,
    clip_start,
    clip_end,
    qkv_weight,
    out_weight,
    up_weight,
    down_weight,
    vectors,
    qkv_first,
    out_first,
    up_first,
    down_first,
    vector_first,
    qkv_second,
    out_second,
    up_second,
    down_second,
    vector_second,
):
    rows, width = tokens.shape
    device = lax.axis_index("dev")
    devices = lax.axis_size("dev")
    heads = width // HD
    reach = (rows + CLIP - 2) // rows
    base = reach * rows
    window_first = device * rows - base
    shards = (qkv_weight, out_weight, up_weight, down_weight, vectors)
    vector_part = jnp.pad(vectors.T, ((0, 0), (0, LANE - vectors.shape[0])))
    spans = jnp.pad(jnp.stack([clip_start, clip_end]), ((0, 6), (0, 0)))
    fulls, (tokens_window, spans_window) = gather([qkv_weight, vector_part, out_weight, up_weight, down_weight], [tokens, spans], devices)
    dims = chip_axes(devices)
    qkv_full = fulls[0].reshape(-1, width, width)
    vector_full = fulls[1].reshape(width, LANE)[:, : vectors.shape[0]].T.astype(jnp.float32)
    out_full = fulls[2].reshape(width, width)
    up_full = fulls[3].reshape(width, -1)
    down_full = fulls[4].reshape(-1, width)
    tokens_window = tokens_window.reshape(-1, width)
    spans_window = spans_window.transpose(1, 0, 2).reshape(8, -1)
    places = window_first + jnp.arange(spans_window.shape[1], dtype=jnp.int32)
    inside = (places >= 0) & (places < devices * rows)
    starts = jnp.where(inside, spans_window[0] - window_first, FAR)
    ends = jnp.where(inside, spans_window[1] - window_first, 0)
    own_start, own_end = clip_start - window_first, clip_end - window_first

    tq, tk = FORWARD_TILES
    forward_bounds = jnp.stack([own_start[::tq] // tk, (own_end[tq - 1 :: tq] + tk - 1) // tk], axis=1).reshape(-1)
    rq, rk = QUERY_TILES
    query_bounds = jnp.stack([own_start[::rq] // rk, (own_end[rq - 1 :: rq] + rk - 1) // rk], axis=1).reshape(-1)
    sk, sq = KEY_TILES
    last_keys = base + sk - 1 + jnp.arange(rows // sk, dtype=jnp.int32) * sk
    last_tiles = jnp.sum((starts[::sq][None, :] <= last_keys[:, None]).astype(jnp.int32), axis=1)
    first_tiles = own_start[::sk] // sq
    last_tiles = first_tiles + jnp.sum(((starts[::sq][None, :] <= last_keys[:, None]) & (jnp.arange(starts.shape[0] // sq)[None, :] >= first_tiles[:, None])).astype(jnp.int32), axis=1)
    key_bounds = jnp.stack([first_tiles, last_tiles], axis=1).reshape(-1)
    needed = jnp.stack([own_start[0] // PROJECT_TILE, (jnp.sum((inside & (starts < base + rows)).astype(jnp.int32)) + jnp.maximum(-window_first, 0) + PROJECT_TILE - 1) // PROJECT_TILE])

    query_window, key_window, value_window = project(tokens_window, vector_full, qkv_full, needed, PROJECT_TILE)
    lower, upper = own_start[:, None], own_end[:, None]
    mixed, lse = attend(query_window, key_window, value_window, lower, upper, forward_bounds, tq, tk, GROUP)
    up_bias = vector_full[8:].reshape(1, -1)
    (result, grad_middle, grad_mixed, delta, grad_out, grad_up, grad_down, middle_rows, bias_row) = middle_block(
        tokens, mixed, cotangent, vector_full, up_bias, out_full, up_full, down_full, MIDDLE_TILE, MIDDLE_CHUNK
    )
    table = jnp.concatenate([lse[:, :heads], delta[:, :heads]], axis=1).T
    spread = lambda grad, lead=(): grad.reshape(lead + dims + (2, grad.shape[len(lead)] // devices, grad.shape[-1]))
    (up_owned, down_owned, out_owned), (grad_window, table_window) = scatter(
        [spread(grad_up), spread(grad_down), spread(grad_out)], [grad_mixed, table], devices, EXCHANGE_ORDERS, 1
    )
    grad_window = grad_window.reshape(-1, width)
    table_window = table_window.transpose(1, 0, 2).reshape(2 * heads, -1)
    groups = heads // (2 * GROUP)
    lse_window = table_window[:heads].reshape(groups, 2 * GROUP, -1)
    delta_window = table_window[heads:].reshape(groups, 2 * GROUP, -1)
    grad_query = query_grad(query_window, grad_mixed, key_window, value_window, lse, delta, lower, upper, query_bounds, rq, rk, GROUP)
    grad_keys, grad_values = key_grad(
        key_window, value_window, query_window, grad_window, lse_window, delta_window,
        starts[None, :], ends[None, :], key_bounds, base, rows, sk, sq, GROUP,
    )
    grad_tokens, grad_qkv, last_rows = last_block(
        tokens, grad_middle, grad_query, grad_keys, grad_values, vector_full, qkv_full, LAST_TILE
    )
    grad_vectors = jnp.concatenate([last_rows[:4], middle_rows[:4], bias_row.reshape(-1, width)], axis=0)
    vector_rows = grad_vectors.reshape(vectors.shape[0], devices, -1).transpose(1, 0, 2).reshape(devices, -1)
    vector_rows = jnp.pad(vector_rows, ((0, 0), (0, 8 * LANE - vector_rows.shape[1]))).reshape(dims + (2, 8, LANE))
    (qkv_owned, vector_owned), _ = scatter([spread(grad_qkv, (3,)), vector_rows], [], devices, SCATTER_ORDERS, 2)
    vector_owned = vector_owned.reshape(-1)[: vectors.size].reshape(vectors.shape)
    owned = (qkv_owned, out_owned, up_owned, down_owned, vector_owned)
    firsts = (qkv_first, out_first, up_first, down_first, vector_first)
    seconds = (qkv_second, out_second, up_second, down_second, vector_second)
    stepped = [adamw_step(*four) for four in zip(shards, owned, firsts, seconds)]
    return (result, grad_tokens) + tuple(stepped[place][kind] for kind in range(3) for place in range(5))


def solution(mesh):
    in_specs = (
        P("dev", None),
        P("dev", None),
        P("dev"),
        P("dev"),
        P(None, "dev", None),
        P("dev", None),
        P("dev", None),
        P("dev", None),
        P(None, "dev"),
        P(None, "dev", None),
        P("dev", None),
        P("dev", None),
        P("dev", None),
        P(None, "dev"),
        P(None, "dev", None),
        P("dev", None),
        P("dev", None),
        P("dev", None),
        P(None, "dev"),
    )
    out_specs = (
        P("dev", None),
        P("dev", None),
        P(None, "dev", None),
        P("dev", None),
        P("dev", None),
        P("dev", None),
        P(None, "dev"),
        P(None, "dev", None),
        P("dev", None),
        P("dev", None),
        P("dev", None),
        P(None, "dev"),
        P(None, "dev", None),
        P("dev", None),
        P("dev", None),
        P("dev", None),
        P(None, "dev"),
    )
    return jax.shard_map(
        per_device, mesh=mesh, in_specs=in_specs, out_specs=out_specs, check_vma=False
    )
```

```python
import functools

import jax
import jax.numpy as jnp
from jax import lax
from jax.experimental import pallas as pl
from jax.experimental.pallas import tpu as pltpu
from jax.sharding import PartitionSpec as P

HD = 64
CLIP = 1500
STEP = 10
LANE = 128
FAR = 1 << 30
SQRT_HALF = 0.7071067811865476
INV_SQRT_TWO_PI = 0.3989422804014327


beta_one = 0.9
beta_two = 0.999
learn_rate = 0.02
weight_decay = 0.1
adam_eps = 1e-08
norm_eps = 1e-05
masked_score = -1e30
FORWARD_TILES = (256, 256)
QUERY_TILES = (256, 256)
KEY_TILES = (256, 256)
PROJECT_TILE = 768
MIDDLE_TILE = 256
MIDDLE_CHUNK = 512
LAST_TILE = 256
GROUP = 3
CHUNK_BYTES = 40000
PER_STEP = 4
HALO_START = 0
HALO_PASS = 3
GATHER_ORDERS = ((0, 1, 2), (0, 2, 1))
SCATTER_ORDERS = ((2, 1, 0), (1, 2, 0))
EXCHANGE_ORDERS = ((1, 2, 0), (1, 2, 0), (2, 1, 0))
SCATTER_PASS = 3
GATHER_LEVELS = (0, 1, 2, 3)
SCATTER_LEVELS = (0, 1, 2, 3, 4)
NT = (((1,), (1,)), ((), ()))
NN = (((1,), (0,)), ((), ()))


def shifted(value, axis, steps):
    count = lax.axis_size(axis)
    initial, last = (max(0, -steps), min(count, count - steps))
    return lax.ppermute(value, axis, [(source, source + steps) for source in range(initial, last)])


def dot(a, b, dims=NN):
    return lax.dot_general(a, b, dims, preferred_element_type=jnp.float32)


def stacked(pair, scale):
    lane = lax.broadcasted_iota(jnp.int32, pair.shape, 1)
    zero = jnp.zeros_like(pair)
    if scale is not None:
        pair = pair * jnp.asarray(scale, pair.dtype)
    return jnp.concatenate([jnp.where(lane < HD, pair, zero), jnp.where(lane >= HD, pair, zero)], axis=0)


def unstacked(both):
    rows = both.shape[0] // 2
    lane = lax.broadcasted_iota(jnp.int32, (rows, LANE), 1)
    return jnp.where(lane < HD, both[:rows], both[rows:])


def joined(turned):
    rows = turned.shape[1] // 2
    return jnp.concatenate([turned[:HD, :rows], turned[HD:, rows:]], axis=0).T


def forward_kernel(tq, tk, pairs, bounds, lower, upper, q_ref, k_ref, v_ref, o_ref, lse_ref, qs, peak, total, acc):
    tiles = q_ref.shape[0] // tq

    def one_tile(tile, none):
        rows = pl.ds(pl.multiple_of(tile * tq, tq), tq)
        for pair in range(pairs):
            qs[pair] = stacked(q_ref[rows, pair * LANE : (pair + 1) * LANE], HD ** -0.5)
        peak[...] = jnp.full_like(peak, masked_score)
        total[...] = jnp.zeros_like(total)
        acc[...] = jnp.zeros_like(acc)
        low, high = lower[:, rows], upper[:, rows]

        def step(key_tile, none):
            first = pl.multiple_of(key_tile * tk, tk)
            places = first + lax.broadcasted_iota(jnp.int32, (tk, tq), 0)
            bias = jnp.where((places >= low) & (places < high), 0.0, masked_score)
            bias = jnp.concatenate([bias, bias], axis=1)
            for pair in range(pairs):
                lanes = slice(pair * LANE, (pair + 1) * LANE)
                scores = dot(k_ref[pl.ds(first, tk), lanes], qs[pair], NT) + bias
                old = peak[pair]
                new = jnp.maximum(old, jnp.max(scores, axis=0, keepdims=True))
                peak[pair] = new
                weights = jnp.exp(scores - new)
                scale = jnp.exp(old - new)
                total[pair] = total[pair] * scale + jnp.sum(weights, axis=0, keepdims=True)
                acc[pair] = acc[pair] * scale + dot(v_ref[pl.ds(first, tk), lanes].T, weights.astype(jnp.bfloat16))
            return none

        lax.fori_loop(bounds[2 * tile], bounds[2 * tile + 1], step, 0)
        for pair in range(pairs):
            o_ref[rows, pair * LANE : (pair + 1) * LANE] = joined(acc[pair] / total[pair]).astype(o_ref.dtype)
            logs = peak[pair] + jnp.log(total[pair])
            lse_ref[0, 2 * pair : 2 * pair + 1, rows] = logs[:, :tq]
            lse_ref[0, 2 * pair + 1 : 2 * pair + 2, rows] = logs[:, tq:]
        return none

    lax.fori_loop(0, tiles, one_tile, 0)


def attend(query, keys, values, lower, upper, bounds, tq, tk, pairs):
    rows, (window, width) = lower.shape[1], keys.shape
    middle = window // rows // 2
    lanes = pairs * LANE
    far = lambda: pl.BlockSpec((window, lanes), lambda g, b: (0, g))
    line = lambda: pl.BlockSpec((1, rows), lambda g, b: (0, 0))
    return pl.pallas_call(
        functools.partial(forward_kernel, tq, tk, pairs),
        grid_spec=pltpu.PrefetchScalarGridSpec(
            num_scalar_prefetch=1, grid=(width // lanes,),
            in_specs=[line(), line(), pl.BlockSpec((rows, lanes), lambda g, b: (middle, g)), far(), far()],
            out_specs=[
                pl.BlockSpec((rows, lanes), lambda g, b: (0, g)),
                pl.BlockSpec((1, 2 * pairs, rows), lambda g, b: (g, 0, 0)),
            ],
            scratch_shapes=[
                pltpu.VMEM((pairs, 2 * tq, LANE), jnp.bfloat16),
                pltpu.VMEM((pairs, 1, 2 * tq), jnp.float32),
                pltpu.VMEM((pairs, 1, 2 * tq), jnp.float32),
                pltpu.VMEM((pairs, LANE, 2 * tq), jnp.float32),
            ],
        ),
        out_shape=[
            jax.ShapeDtypeStruct((rows, width), jnp.bfloat16),
            jax.ShapeDtypeStruct((width // lanes, 2 * pairs, rows), jnp.float32),
        ],
        name="attend",
    )(bounds, lower, upper, query, keys, values)


def query_grad_kernel(tq, tk, pairs, bounds, lower, upper, q_ref, g_ref, k_ref, v_ref, lse_ref, delta_ref, dq_ref, qs, gs, acc):
    tiles = q_ref.shape[0] // tq

    def one_tile(tile, none):
        rows = pl.ds(pl.multiple_of(tile * tq, tq), tq)
        logs, deltas = [], []
        for pair in range(pairs):
            lanes = slice(pair * LANE, (pair + 1) * LANE)
            qs[pair] = stacked(q_ref[rows, lanes], HD ** -0.5)
            gs[pair] = stacked(g_ref[rows, lanes], None)
            for held, ref in ((logs, lse_ref), (deltas, delta_ref)):
                halves = [ref[0, 2 * pair + half : 2 * pair + half + 1, rows] for half in range(2)]
                held.append(jnp.concatenate(halves, axis=1))
        acc[...] = jnp.zeros_like(acc)
        low, high = lower[:, rows], upper[:, rows]

        def step(key_tile, none):
            first = pl.multiple_of(key_tile * tk, tk)
            places = first + lax.broadcasted_iota(jnp.int32, (tk, tq), 0)
            bias = jnp.where((places >= low) & (places < high), 0.0, masked_score)
            bias = jnp.concatenate([bias, bias], axis=1)
            for pair in range(pairs):
                lanes = slice(pair * LANE, (pair + 1) * LANE)
                keys = k_ref[pl.ds(first, tk), lanes]
                probs = jnp.exp(dot(keys, qs[pair], NT) + bias - logs[pair])
                grad_probs = dot(v_ref[pl.ds(first, tk), lanes], gs[pair], NT)
                grad_scores = (probs * (grad_probs - deltas[pair])).astype(jnp.bfloat16)
                acc[pair] += dot(keys.T, grad_scores)
            return none

        lax.fori_loop(bounds[2 * tile], bounds[2 * tile + 1], step, 0)
        for pair in range(pairs):
            dq_ref[rows, pair * LANE : (pair + 1) * LANE] = joined(acc[pair] * HD ** -0.5).astype(dq_ref.dtype)
        return none

    lax.fori_loop(0, tiles, one_tile, 0)


def query_grad(query, grad, keys, values, lse, delta, lower, upper, bounds, tq, tk, pairs):
    (rows, width), window = grad.shape, keys.shape[0]
    middle = window // rows // 2
    lanes = pairs * LANE
    own = lambda at=0: pl.BlockSpec((rows, lanes), lambda g, b: (at, g))
    far = lambda: pl.BlockSpec((window, lanes), lambda g, b: (0, g))
    line = lambda: pl.BlockSpec((1, rows), lambda g, b: (0, 0))
    heads = lambda: pl.BlockSpec((1, 2 * pairs, rows), lambda g, b: (g, 0, 0))
    return pl.pallas_call(
        functools.partial(query_grad_kernel, tq, tk, pairs),
        grid_spec=pltpu.PrefetchScalarGridSpec(
            num_scalar_prefetch=1, grid=(width // lanes,),
            in_specs=[line(), line(), own(middle), own(), far(), far(), heads(), heads()],
            out_specs=own(),
            scratch_shapes=[
                pltpu.VMEM((pairs, 2 * tq, LANE), jnp.bfloat16),
                pltpu.VMEM((pairs, 2 * tq, LANE), jnp.bfloat16),
                pltpu.VMEM((pairs, LANE, 2 * tq), jnp.float32),
            ],
        ),
        out_shape=jax.ShapeDtypeStruct((rows, width), jnp.bfloat16),
        name="query_grad",
    )(bounds, lower, upper, query, grad, keys, values, lse, delta)


def key_grad_kernel(tk, tq, pairs, base, bounds, lower, upper, k_ref, v_ref, q_ref, g_ref, lse_ref, delta_ref, dk_ref, dv_ref, ks, vs, acc):
    tiles = k_ref.shape[0] // tk

    def one_tile(tile, none):
        rows = pl.ds(pl.multiple_of(tile * tk, tk), tk)
        for pair in range(pairs):
            lanes = slice(pair * LANE, (pair + 1) * LANE)
            ks[pair] = stacked(k_ref[rows, lanes], HD ** -0.5)
            vs[pair] = stacked(v_ref[rows, lanes], None)
        acc[...] = jnp.zeros_like(acc)

        def step(query_tile, none):
            first = pl.multiple_of(query_tile * tq, tq)
            here = pl.ds(first, tq)
            places = base + tile * tk + lax.broadcasted_iota(jnp.int32, (tk, tq), 0)
            bias = jnp.where((places >= lower[:, here]) & (places < upper[:, here]), 0.0, masked_score)
            for pair in range(pairs):
                lanes = slice(pair * LANE, (pair + 1) * LANE)
                queries, grads = q_ref[here, lanes], g_ref[here, lanes]
                scores = dot(ks[pair], queries, NT)
                grad_probs = dot(vs[pair], grads, NT)
                probs, grad_scores = [], []
                for half in range(2):
                    part = slice(half * tk, (half + 1) * tk)
                    head = slice(2 * pair + half, 2 * pair + half + 1)
                    prob = jnp.exp(scores[part] + bias - lse_ref[0, head, here])
                    probs.append(prob.astype(jnp.bfloat16))
                    grad_scores.append((prob * (grad_probs[part] - delta_ref[0, head, here])).astype(jnp.bfloat16))
                acc[pair, :, :LANE] += dot(jnp.concatenate(grad_scores, axis=0), queries)
                acc[pair, :, LANE:] += dot(jnp.concatenate(probs, axis=0), grads)
            return none

        lax.fori_loop(bounds[2 * tile], bounds[2 * tile + 1], step, 0)
        for pair in range(pairs):
            lanes = slice(pair * LANE, (pair + 1) * LANE)
            dk_ref[rows, lanes] = (unstacked(acc[pair, :, :LANE]) * HD ** -0.5).astype(dk_ref.dtype)
            dv_ref[rows, lanes] = unstacked(acc[pair, :, LANE:]).astype(dv_ref.dtype)
        return none

    lax.fori_loop(0, tiles, one_tile, 0)


def key_grad(keys, values, query, grad, lse, delta, lower, upper, bounds, base, rows, tk, tq, pairs):
    window, width = query.shape
    middle = base // rows
    lanes = pairs * LANE
    own = lambda at=0: pl.BlockSpec((rows, lanes), lambda g, b: (at, g))
    far = lambda: pl.BlockSpec((window, lanes), lambda g, b: (0, g))
    line = lambda: pl.BlockSpec((1, window), lambda g, b: (0, 0))
    heads = lambda: pl.BlockSpec((1, 2 * pairs, window), lambda g, b: (g, 0, 0))
    return pl.pallas_call(
        functools.partial(key_grad_kernel, tk, tq, pairs, base),
        grid_spec=pltpu.PrefetchScalarGridSpec(
            num_scalar_prefetch=1, grid=(width // lanes,),
            in_specs=[line(), line(), own(middle), own(middle), far(), far(), heads(), heads()],
            out_specs=[own(), own()],
            scratch_shapes=[
                pltpu.VMEM((pairs, 2 * tk, LANE), jnp.bfloat16),
                pltpu.VMEM((pairs, 2 * tk, LANE), jnp.bfloat16),
                pltpu.VMEM((pairs, 2 * tk, 2 * LANE), jnp.float32),
            ],
        ),
        out_shape=[jax.ShapeDtypeStruct((rows, width), jnp.bfloat16)] * 2,
        name="key_grad",
    )(bounds, lower, upper, keys, values, query, grad, lse, delta)


def units(values):
    centre = values - jnp.mean(values, axis=-1, keepdims=True)
    inverse = lax.rsqrt(jnp.mean(centre * centre, axis=-1, keepdims=True) + norm_eps)
    return centre * inverse, inverse


def norm_pull(grad_output, unit, inverse, gain):
    grad_unit = grad_output * gain
    first = jnp.mean(grad_unit, axis=-1, keepdims=True)
    second = jnp.mean(grad_unit * unit, axis=-1, keepdims=True)
    return inverse * (grad_unit - first - unit * second)


def row_sum(values):
    return jnp.sum(values, axis=0, keepdims=True)


def gelu_pair(hidden):
    inner = 0.5 + 0.5 * lax.erf(hidden * SQRT_HALF)
    slope = inner + hidden * (jnp.exp(-0.5 * hidden * hidden) * INV_SQRT_TWO_PI)
    return hidden * inner, slope


def project_kernel(tile, active, tokens, vectors, weights, query, keys, values):
    place = pl.program_id(0)
    needed = (place >= active[0]) & (place < active[1])

    @pl.when(needed)
    def _():
        unit = units(tokens[...].astype(jnp.float32))[0]
        normed = (unit * vectors[0:1, :] + vectors[1:2, :]).astype(jnp.bfloat16)
        query[...] = (dot(normed, weights[0]) + vectors[2:3, :]).astype(query.dtype)
        keys[...] = dot(normed, weights[1]).astype(keys.dtype)
        values[...] = (dot(normed, weights[2]) + vectors[3:4, :]).astype(values.dtype)

    @pl.when(jnp.logical_not(needed))
    def _():
        for out in (query, keys, values):
            out[...] = jnp.zeros_like(out)


def project(tokens, vectors, weights, active, tile):
    rows, width = tokens.shape
    block = lambda: pl.BlockSpec((tile, width), lambda i, b: (i, 0))
    return pl.pallas_call(
        functools.partial(project_kernel, tile),
        grid_spec=pltpu.PrefetchScalarGridSpec(
            num_scalar_prefetch=1, grid=(rows // tile,),
            in_specs=[
                block(),
                pl.BlockSpec(vectors.shape, lambda i, b: (0, 0)),
                pl.BlockSpec(weights.shape, lambda i, b: (0, 0, 0)),
            ],
            out_specs=[block(), block(), block()],
        ),
        out_shape=[jax.ShapeDtypeStruct((rows, width), jnp.bfloat16)] * 3,
        name="project",
    )(active, tokens, vectors, weights)


def middle_kernel(tile, tokens, mixed, cotangent, vectors, up_bias, out_weight, up_weight, down_weight,
                  result, grad_middle, grad_mixed, delta, grad_out, grad_up, grad_down, grad_rows, grad_bias,
                  middle, normed, turned, total, back, actives, hiddens):
    place, count = pl.program_id(0), pl.num_programs(0)
    rows = tokens.shape[0]
    parts = [slice(i, i + tile) for i in range(0, rows, tile)]

    @pl.when(place == 0)
    def _():
        for part in parts:
            branch = dot(mixed[part, :], out_weight[...]) + vectors[4:5, :]
            wide = tokens[part, :].astype(jnp.float32) + branch
            middle[part, :] = wide
            unit = units(wide)[0]
            low = (unit * vectors[5:6, :] + vectors[6:7, :]).astype(jnp.bfloat16)
            normed[part, :] = low
            turned[:, part] = low.T
            total[part, :] = wide + vectors[7:8, :]
        back[...] = jnp.zeros_like(back)

    bias = jnp.zeros_like(grad_bias)
    for part in parts:
        hidden = dot(normed[part, :], up_weight[...]) + up_bias[...]
        wide, slope = gelu_pair(hidden)
        active = wide.astype(jnp.bfloat16)
        grad_active = dot(cotangent[part, :], down_weight[...], NT)
        grad_hidden = (grad_active * slope).astype(jnp.bfloat16)
        actives[part, :] = active
        hiddens[part, :] = grad_hidden
        bias += row_sum(grad_hidden.astype(jnp.float32))
        total[part, :] += dot(active, down_weight[...])
        back[part, :] += dot(grad_hidden, up_weight[...], NT)
    grad_bias[...] = bias
    grad_up[...] = dot(turned[...], hiddens[...]).astype(grad_up.dtype)
    grad_down[...] = dot(actives[...], cotangent[...], (((0,), (0,)), ((), ()))).astype(grad_down.dtype)

    @pl.when(place == count - 1)
    def _():
        sums = [jnp.zeros((1, tokens.shape[1]), jnp.float32) for _ in range(4)]
        for part in parts:
            result[part, :] = total[part, :].astype(result.dtype)
            unit, inverse = units(middle[part, :])
            incoming = back[part, :]
            wide = cotangent[part, :].astype(jnp.float32)
            grad = wide + norm_pull(incoming, unit, inverse, vectors[5:6, :])
            grad_middle[part, :] = grad
            branch = grad.astype(jnp.bfloat16)
            turned[:, part] = mixed[part, :].T
            hiddens_low = dot(branch, out_weight[...], NT).astype(jnp.bfloat16)
            grad_mixed[part, :] = hiddens_low
            product = hiddens_low.astype(jnp.float32) * mixed[part, :].astype(jnp.float32)
            delta[part, :] = head_sums(product)
            normed[part, :] = branch
            sums[0] += row_sum(branch.astype(jnp.float32))
            sums[1] += row_sum(incoming * unit)
            sums[2] += row_sum(incoming)
            sums[3] += row_sum(wide)
        grad_out[...] = dot(turned[...], normed[...]).astype(grad_out.dtype)
        grad_rows[...] = jnp.concatenate(sums + [jnp.zeros((4, tokens.shape[1]), jnp.float32)], axis=0)


def head_sums(product):
    rows, width = product.shape
    lane = lax.broadcasted_iota(jnp.int32, (rows, LANE), 1)
    table = jnp.zeros((rows, LANE), jnp.float32)
    for pair in range(width // LANE):
        piece = product[:, pair * LANE : (pair + 1) * LANE]
        first = jnp.sum(jnp.where(lane < HD, piece, 0.0), axis=1, keepdims=True)
        second = jnp.sum(jnp.where(lane >= HD, piece, 0.0), axis=1, keepdims=True)
        table = jnp.where(lane == 2 * pair, first, table)
        table = jnp.where(lane == 2 * pair + 1, second, table)
    return table


def middle_block(tokens, mixed, cotangent, vectors, up_bias, out_weight, up_weight, down_weight, tile, chunk):
    rows, width = tokens.shape
    hidden = up_weight.shape[1]
    whole = lambda shape: pl.BlockSpec(shape, lambda i: (0,) * len(shape))
    across = lambda r: pl.BlockSpec((r, chunk), lambda i: (0, i))
    down = lambda: pl.BlockSpec((chunk, width), lambda i: (i, 0))
    full = (rows, width)
    return pl.pallas_call(
        functools.partial(middle_kernel, tile),
        grid=(hidden // chunk,),
        in_specs=[whole(full), whole(full), whole(full), whole(vectors.shape), across(1), whole((width, width)), across(width), down()],
        out_specs=[whole(full), whole(full), whole(full), whole((rows, LANE)), whole((width, width)), across(width), down(), whole((8, width)), across(1)],
        out_shape=[
            jax.ShapeDtypeStruct(full, jnp.bfloat16),
            jax.ShapeDtypeStruct(full, jnp.float32),
            jax.ShapeDtypeStruct(full, jnp.bfloat16),
            jax.ShapeDtypeStruct((rows, LANE), jnp.float32),
            jax.ShapeDtypeStruct((width, width), jnp.bfloat16),
            jax.ShapeDtypeStruct((width, hidden), jnp.bfloat16),
            jax.ShapeDtypeStruct((hidden, width), jnp.bfloat16),
            jax.ShapeDtypeStruct((8, width), jnp.float32),
            jax.ShapeDtypeStruct((1, hidden), jnp.float32),
        ],
        scratch_shapes=[
            pltpu.VMEM(full, jnp.float32),
            pltpu.VMEM(full, jnp.bfloat16),
            pltpu.VMEM((width, rows), jnp.bfloat16),
            pltpu.VMEM(full, jnp.float32),
            pltpu.VMEM(full, jnp.float32),
            pltpu.VMEM((rows, chunk), jnp.bfloat16),
            pltpu.VMEM((rows, chunk), jnp.bfloat16),
        ],
        name="middle",
    )(tokens, mixed, cotangent, vectors, up_bias, out_weight, up_weight, down_weight)


def last_kernel(tile, tokens, grad_middle, grad_query, grad_keys, grad_values, vectors, weights,
                grad_tokens, grad_qkv, grad_rows, turned):
    rows, width = tokens.shape
    sums = [jnp.zeros((1, width), jnp.float32) for _ in range(4)]
    for first in range(0, rows, tile):
        part = slice(first, first + tile)
        unit, inverse = units(tokens[part, :].astype(jnp.float32))
        turned[:, part] = (unit * vectors[0:1, :] + vectors[1:2, :]).astype(jnp.bfloat16).T
        incoming = dot(grad_query[part, :], weights[0], NT)
        incoming += dot(grad_keys[part, :], weights[1], NT)
        incoming += dot(grad_values[part, :], weights[2], NT)
        grad_tokens[part, :] = grad_middle[part, :] + norm_pull(incoming, unit, inverse, vectors[0:1, :])
        sums[0] += row_sum(incoming * unit)
        sums[1] += row_sum(incoming)
        sums[2] += row_sum(grad_query[part, :].astype(jnp.float32))
        sums[3] += row_sum(grad_values[part, :].astype(jnp.float32))
    for place, grad in enumerate((grad_query, grad_keys, grad_values)):
        grad_qkv[place] = dot(turned[...], grad[...]).astype(grad_qkv.dtype)
    grad_rows[...] = jnp.concatenate(sums + [jnp.zeros((4, width), jnp.float32)], axis=0)


def last_block(tokens, grad_middle, grad_query, grad_keys, grad_values, vectors, weights, tile):
    rows, width = tokens.shape
    return pl.pallas_call(
        functools.partial(last_kernel, tile),
        out_shape=[
            jax.ShapeDtypeStruct((rows, width), jnp.float32),
            jax.ShapeDtypeStruct(weights.shape, jnp.bfloat16),
            jax.ShapeDtypeStruct((8, width), jnp.float32),
        ],
        scratch_shapes=[pltpu.VMEM((width, rows), jnp.bfloat16)],
        name="last",
    )(tokens, grad_middle, grad_query, grad_keys, grad_values, vectors, weights)


def chip_axes(devices):
    chips = devices // 2
    return {16: (4, 2, 2), 64: (4, 4, 4)}.get(chips, (chips, 1, 1))


class Place:
    def __init__(self, dims):
        self.dims = dims
        self.me = lax.axis_index("dev")
        self.core = lax.rem(self.me, 2)
        chip = self.me // 2
        self.at = (chip // (dims[1] * dims[2]), lax.rem(chip // dims[2], dims[1]), lax.rem(chip, dims[2]))
        self.partner = self.me + 1 - 2 * self.core

    def peer(self, axis, step):
        there = lax.rem(self.at[axis] + step, self.dims[axis])
        at = [there if a == axis else self.at[a] for a in range(3)]
        return ((at[0] * self.dims[1] + at[1]) * self.dims[2] + at[2]) * 2 + self.core, there

    def peers(self):
        return [self.partner] + [self.peer(axis, step)[0] for axis in range(3) for step in range(1, self.dims[axis])]


def remote(source, target, send, recv, device):
    return pltpu.make_async_remote_copy(
        src_ref=source, dst_ref=target, send_sem=send, recv_sem=recv,
        device_id=(device,), device_id_type=pl.DeviceIdType.MESH,
    )


def greet(peers, around=None, devices=0):
    barrier = pltpu.get_barrier_semaphore()
    count = len(peers)
    for peer in peers:
        pl.semaphore_signal(barrier, inc=1, device_id=(peer,), device_id_type=pl.DeviceIdType.MESH)
    if around is not None:
        for other in (around - 2, around + 2):
            there = (other >= 0) & (other < devices)
            count = count + there.astype(jnp.int32)

            @pl.when(there)
            def _():
                pl.semaphore_signal(barrier, inc=1, device_id=(other,), device_id_type=pl.DeviceIdType.MESH)

    pl.semaphore_wait(barrier, count)


class Halo:
    def __init__(self, place, devices, own, window, send, recv, local):
        self.place, self.devices, self.own, self.window = place, devices, own, window
        self.send, self.recv, self.local = send, recv, local
        me, core = place.me, place.core
        self.above, self.below = me + 2 < devices, me >= 2
        self.up = remote(own, window.at[0], send.at[0], recv.at[0], me + 2)
        self.down = remote(own, window.at[4], send.at[1], recv.at[1], me - 2)
        side = jnp.where(core == 0, 1, 3)
        self.across = remote(own, window.at[side], send.at[2], recv.at[2], place.partner)
        self.kept = jnp.where(core == 0, 4, 0)
        self.relay = remote(window.at[self.kept], window.at[4 - side], send.at[3], recv.at[3], place.partner)
        self.keep = pltpu.make_async_copy(own, window.at[2], local)

    def start(self):
        pl.when(self.above)(self.up.start)
        pl.when(self.below)(self.down.start)
        self.across.start()
        self.keep.start()

    def pass_on(self):
        pl.when(self.below)(self.up.wait_recv)
        pl.when(self.above)(self.down.wait_recv)
        even = self.place.core == 0
        self.relays = jnp.where(even, self.above, self.below)
        pl.when(self.relays)(self.relay.start)

    def finish(self):
        even = self.place.core == 0
        comes = jnp.where(even, self.below, self.above)
        self.across.wait_recv()
        pl.when(comes)(self.relay.wait_recv)
        self.keep.wait()
        pl.when(self.above)(self.up.wait_send)
        pl.when(self.below)(self.down.wait_send)
        self.across.wait_send()
        pl.when(self.relays)(self.relay.wait_send)


def gather_kernel(dims, devices, chunks, orders, arrays, halos, *refs):
    shards, owns = refs[:arrays], refs[arrays : arrays + halos]
    fulls = refs[arrays + halos : 2 * arrays + halos]
    windows = refs[2 * arrays + halos : 2 * (arrays + halos)]
    scratch = refs[2 * (arrays + halos) :]
    wides, shards = shards, scratch[:arrays]
    send, recv, local, halo_send, halo_recv, halo_local = scratch[arrays:]
    place = Place(dims)
    for wide, shard in zip(wides, shards):
        shard[...] = wide[...].astype(shard.dtype)
    greet(place.peers(), place.me, devices)
    parts = [
        Halo(place, devices, owns[i], windows[i], halo_send.at[i], halo_recv.at[i], halo_local.at[i])
        for i in range(halos)
    ]
    count = len(chunks)
    started = {}

    def stage(number, level):
        array, lead, lanes = chunks[number]
        shard, full = shards[array], fulls[array]
        front = () if lead is None else (lead,)
        source = shard.at[front + (slice(None), lanes)] if front else shard.at[:, lanes]
        order = orders[number]
        done = order[: min(level, 3)]
        index = tuple(slice(None) if axis in done else place.at[axis] for axis in range(3))
        view = lambda index, core: full.at[front + index + (core, slice(None), lanes)]
        if level == 0:
            mine = pltpu.make_async_copy(source, view(index, place.core), local.at[number])
            mine.start()
            started[number] = [mine]
        else:
            for copy in started[number, level - 1]:
                copy.wait_recv()
            if level == 1:
                started[number][0].wait()
            source = view(index, place.core)
        copies = []
        if level == 3:
            copies.append(remote(source, source, send.at[number, 0], recv.at[number, 0], place.partner))
        else:
            base = 1 + sum(dims[axis] - 1 for axis in order[:level])
            for step in range(1, dims[order[level]]):
                slot = base + step - 1
                device = place.peer(order[level], step)[0]
                target = view(index, place.core)
                copies.append(remote(source, target, send.at[number, slot], recv.at[number, slot], device))
        for copy in copies:
            copy.start()
        started[number, level] = copies

    steps = -(-count // PER_STEP)
    for time in range(steps + 3):
        for level in GATHER_LEVELS:
            for number in range((time - level) * PER_STEP, (time - level + 1) * PER_STEP):
                if 0 <= number < count:
                    stage(number, level)
        if time == HALO_START:
            for part in parts:
                part.start()
        if time == min(HALO_PASS, steps + 2):
            for part in parts:
                part.pass_on()
    for number in range(count):
        for copy in started[number, 3]:
            copy.wait_recv()
        for level in range(4):
            for copy in started[number, level]:
                copy.wait_send()
    for part in parts:
        part.finish()


def gather(shards, owns, devices):
    dims = chip_axes(devices)
    chunks = []
    for array, shard in enumerate(shards):
        lanes = shard.shape[-1]
        if shard.ndim == 3:
            chunks += [(array, lead, slice(0, lanes)) for lead in range(shard.shape[0])]
        else:
            wide = min(lanes, max(CHUNK_BYTES // (2 * shard.shape[0]) // LANE * LANE, LANE))
            wide = max(w for w in range(LANE, wide + 1, LANE) if lanes % w == 0)
            chunks += [(array, None, slice(first, first + wide)) for first in range(0, lanes, wide)]
    orders = [GATHER_ORDERS[number % len(GATHER_ORDERS)] for number in range(len(chunks))]
    slots = 1 + sum(size - 1 for size in dims)
    anywhere = pl.BlockSpec(memory_space=pl.ANY)
    inside = pl.BlockSpec(memory_space=pltpu.VMEM)
    outs = [
        jax.ShapeDtypeStruct(shard.shape[:-2] + dims + (2,) + shard.shape[-2:], jnp.bfloat16) for shard in shards
    ] + [jax.ShapeDtypeStruct((5,) + own.shape, own.dtype) for own in owns]
    done = pl.pallas_call(
        functools.partial(gather_kernel, dims, devices, chunks, orders, len(shards), len(owns)),
        in_specs=[inside] * (len(shards) + len(owns)),
        out_specs=[anywhere] * len(outs),
        out_shape=outs,
        scratch_shapes=[pltpu.VMEM(shard.shape, jnp.bfloat16) for shard in shards] + [
            pltpu.SemaphoreType.DMA((len(chunks), slots)),
            pltpu.SemaphoreType.DMA((len(chunks), slots)),
            pltpu.SemaphoreType.DMA((len(chunks),)),
            pltpu.SemaphoreType.DMA((max(len(owns), 1), 4)),
            pltpu.SemaphoreType.DMA((max(len(owns), 1), 4)),
            pltpu.SemaphoreType.DMA((max(len(owns), 1),)),
        ],
        compiler_params=pltpu.CompilerParams(collective_id=0, has_side_effects=True),
        name="gather",
    )(*shards, *owns)
    return done[: len(shards)], done[len(shards) :]


def scatter_kernel(dims, devices, chunks, arrays, halos, orders, *refs):
    grads, owns = refs[:arrays], refs[arrays : arrays + halos]
    outs = refs[arrays + halos : 2 * arrays + halos]
    windows = refs[2 * arrays + halos : 2 * (arrays + halos)]
    rest = refs[2 * (arrays + halos) :]
    count = len(chunks)
    buffers = [rest[5 * i : 5 * i + 5] for i in range(count)]
    send, recv, local, halo_send, halo_recv, halo_local = rest[5 * count :]
    place = Place(dims)
    if halos:
        greet(place.peers(), place.me, devices)
    else:
        greet(place.peers())
    parts = [
        Halo(place, devices, owns[i], windows[i], halo_send.at[i], halo_recv.at[i], halo_local.at[i])
        for i in range(halos)
    ]
    for part in parts:
        part.start()
    started = {}

    def source(number, core):
        array, lead, lanes = chunks[number]
        front = () if lead is None else (lead,)
        return grads[array].at[front + (slice(None), slice(None), slice(None), core, slice(None), lanes)]

    def spread(shape, one):
        total = 1
        for size in shape:
            total *= size

        def body(flat, none):
            index = []
            for size in reversed(shape):
                index.insert(0, lax.rem(flat, size))
                flat = flat // size
            one(tuple(index))
            return none

        lax.fori_loop(0, total, body, 0)

    def stage(number, level):
        own, first, second, third, fourth = buffers[number]
        order = orders[number]
        held = (own, second, third, fourth)
        copies = []
        if level == 0:
            mine = pltpu.make_async_copy(source(number, place.core), own, local.at[number])
            mine.start()
            started[number] = mine
            copies.append(remote(source(number, 1 - place.core), first, send.at[number, 0], recv.at[number, 0], place.partner))
        else:
            for copy in started[number, level - 1]:
                copy.wait_recv()
            remaining = [axis for axis in range(3) if axis not in order[: level - 1]]
            if level == 1:
                started[number].wait()

                def add(index):
                    total = own[index].astype(jnp.float32) + first[index].astype(jnp.float32)
                    own[index] = total.astype(own.dtype)

                spread(dims, add)
            else:
                combine(number, level)
            axis = order[level - 1]
            base = 1 + sum(dims[a] - 1 for a in order[: level - 1])
            for step in range(1, dims[axis]):
                device, there = place.peer(axis, step)
                where = tuple(there if a == axis else slice(None) for a in remaining)
                slot = base + step - 1
                piece = (own if level == 1 else held[level - 1].at[0]).at[where]
                copies.append(remote(piece, held[level].at[step - 1], send.at[number, slot], recv.at[number, slot], device))
        for copy in copies:
            copy.start()
        started[number, level] = copies

    def combine(number, level):
        own, first, second, third, fourth = buffers[number]
        order = orders[number]
        held = (own, second, third, fourth)
        axis = order[level - 2]
        before = [a for a in range(3) if a not in order[: level - 2]]
        after = [a for a in before if a != axis]
        slots = dims[axis] - 1
        old = own if level == 2 else held[level - 2].at[0]
        new = held[level - 1]
        array, lead, lanes = chunks[number]

        def add(index):
            where = list(index)
            where.insert(before.index(axis), place.at[axis])
            total = old[tuple(where)].astype(jnp.float32)
            for slot in range(slots):
                total += new[(slot,) + index].astype(jnp.float32)
            if level == 4:
                if lead is None:
                    outs[array][:, lanes] = total
                else:
                    outs[array][lead, :, lanes] = total
            else:
                new[(0,) + index] = total.astype(new.dtype)

        if after:
            spread([dims[a] for a in after], add)
        else:
            add(())

    steps = -(-count // PER_STEP)
    for time in range(steps + 4):
        if time == min(SCATTER_PASS, steps + 3):
            for part in parts:
                part.pass_on()
        for level in SCATTER_LEVELS:
            for number in range((time - level) * PER_STEP, (time - level + 1) * PER_STEP):
                if not 0 <= number < count:
                    continue
                if level == 4:
                    for copy in started[number, 3]:
                        copy.wait_recv()
                    combine(number, 4)
                else:
                    stage(number, level)
    for number in range(count):
        for level in range(4):
            for copy in started[number, level]:
                copy.wait_send()
    for part in parts:
        part.finish()


def scatter(grads, owns, devices, orders, identity):
    dims = chip_axes(devices)
    chunks = []
    for array, grad in enumerate(grads):
        rows, lanes = grad.shape[-2:]
        if grad.ndim == 7:
            chunks += [(array, lead, slice(0, lanes)) for lead in range(grad.shape[0])]
        else:
            wide = min(lanes, max(CHUNK_BYTES // (2 * rows) // LANE * LANE, LANE))
            wide = max(w for w in range(LANE, wide + 1, LANE) if lanes % w == 0)
            chunks += [(array, None, slice(first, first + wide)) for first in range(0, lanes, wide)]
    orders = [orders[number % len(orders)] for number in range(len(chunks))]
    scratch = []
    for (array, lead, lanes), order in zip(chunks, orders):
        grad = grads[array]
        piece = (grad.shape[-2], lanes.stop - lanes.start)
        left = [dims[a] for a in range(3)]
        scratch += [pltpu.VMEM(dims + piece, grad.dtype)] * 2
        remaining = [0, 1, 2]
        for axis in order:
            remaining.remove(axis)
            scratch.append(pltpu.VMEM((max(dims[axis] - 1, 1),) + tuple(dims[a] for a in remaining) + piece, grad.dtype))
    slots = 1 + sum(size - 1 for size in dims)
    outs = [jax.ShapeDtypeStruct(grad.shape[:-6] + grad.shape[-2:], jnp.float32) for grad in grads]
    outs += [jax.ShapeDtypeStruct((5,) + own.shape, own.dtype) for own in owns]
    anywhere = pl.BlockSpec(memory_space=pl.ANY)
    inside = pl.BlockSpec(memory_space=pltpu.VMEM)
    done = pl.pallas_call(
        functools.partial(scatter_kernel, dims, devices, chunks, len(grads), len(owns), orders),
        in_specs=[anywhere] * len(grads) + [inside] * len(owns),
        out_specs=[inside] * len(grads) + [anywhere] * len(owns),
        out_shape=outs,
        scratch_shapes=scratch + [
            pltpu.SemaphoreType.DMA((len(chunks), slots)),
            pltpu.SemaphoreType.DMA((len(chunks), slots)),
            pltpu.SemaphoreType.DMA((len(chunks),)),
            pltpu.SemaphoreType.DMA((max(len(owns), 1), 4)),
            pltpu.SemaphoreType.DMA((max(len(owns), 1), 4)),
            pltpu.SemaphoreType.DMA((max(len(owns), 1),)),
        ],
        compiler_params=pltpu.CompilerParams(collective_id=identity, has_side_effects=True),
        name="scatter" if not owns else "exchange",
    )(*grads, *owns)
    return done[: len(grads)], done[len(grads) :]


def adamw_step(master, gradient, first_moment, second_moment):
    first_new = beta_one * first_moment + (1.0 - beta_one) * gradient
    second_new = beta_two * second_moment + (1.0 - beta_two) * gradient * gradient
    fix_one = 1.0 - beta_one**STEP
    fix_two = 1.0 - beta_two**STEP
    update = -learn_rate * (
        first_new / fix_one / (jnp.sqrt(second_new / fix_two) + adam_eps) + weight_decay * master
    )
    return (update, first_new, second_new)


def per_device(
    tokens,
    cotangent,
    clip_start,
    clip_end,
    qkv_weight,
    out_weight,
    up_weight,
    down_weight,
    vectors,
    qkv_first,
    out_first,
    up_first,
    down_first,
    vector_first,
    qkv_second,
    out_second,
    up_second,
    down_second,
    vector_second,
):
    rows, width = tokens.shape
    device = lax.axis_index("dev")
    devices = lax.axis_size("dev")
    heads = width // HD
    reach = (rows + CLIP - 2) // rows
    base = reach * rows
    window_first = device * rows - base
    shards = (qkv_weight, out_weight, up_weight, down_weight, vectors)
    vector_part = jnp.pad(vectors.T, ((0, 0), (0, LANE - vectors.shape[0])))
    spans = jnp.pad(jnp.stack([clip_start, clip_end]), ((0, 6), (0, 0)))
    fulls, (tokens_window, spans_window) = gather([qkv_weight, vector_part, out_weight, up_weight, down_weight], [tokens, spans], devices)
    dims = chip_axes(devices)
    qkv_full = fulls[0].reshape(-1, width, width)
    vector_full = fulls[1].reshape(width, LANE)[:, : vectors.shape[0]].T.astype(jnp.float32)
    out_full = fulls[2].reshape(width, width)
    up_full = fulls[3].reshape(width, -1)
    down_full = fulls[4].reshape(-1, width)
    tokens_window = tokens_window.reshape(-1, width)
    spans_window = spans_window.transpose(1, 0, 2).reshape(8, -1)
    places = window_first + jnp.arange(spans_window.shape[1], dtype=jnp.int32)
    inside = (places >= 0) & (places < devices * rows)
    starts = jnp.where(inside, spans_window[0] - window_first, FAR)
    ends = jnp.where(inside, spans_window[1] - window_first, 0)
    own_start, own_end = clip_start - window_first, clip_end - window_first

    tq, tk = FORWARD_TILES
    forward_bounds = jnp.stack([own_start[::tq] // tk, (own_end[tq - 1 :: tq] + tk - 1) // tk], axis=1).reshape(-1)
    rq, rk = QUERY_TILES
    query_bounds = jnp.stack([own_start[::rq] // rk, (own_end[rq - 1 :: rq] + rk - 1) // rk], axis=1).reshape(-1)
    sk, sq = KEY_TILES
    last_keys = base + sk - 1 + jnp.arange(rows // sk, dtype=jnp.int32) * sk
    last_tiles = jnp.sum((starts[::sq][None, :] <= last_keys[:, None]).astype(jnp.int32), axis=1)
    first_tiles = own_start[::sk] // sq
    last_tiles = first_tiles + jnp.sum(((starts[::sq][None, :] <= last_keys[:, None]) & (jnp.arange(starts.shape[0] // sq)[None, :] >= first_tiles[:, None])).astype(jnp.int32), axis=1)
    key_bounds = jnp.stack([first_tiles, last_tiles], axis=1).reshape(-1)
    needed = jnp.stack([own_start[0] // PROJECT_TILE, (jnp.sum((inside & (starts < base + rows)).astype(jnp.int32)) + jnp.maximum(-window_first, 0) + PROJECT_TILE - 1) // PROJECT_TILE])

    query_window, key_window, value_window = project(tokens_window, vector_full, qkv_full, needed, PROJECT_TILE)
    lower, upper = own_start[None, :], own_end[None, :]
    mixed, lse = attend(query_window, key_window, value_window, lower, upper, forward_bounds, tq, tk, GROUP)
    up_bias = vector_full[8:].reshape(1, -1)
    (result, grad_middle, grad_mixed, delta, grad_out, grad_up, grad_down, middle_rows, bias_row) = middle_block(
        tokens, mixed, cotangent, vector_full, up_bias, out_full, up_full, down_full, MIDDLE_TILE, MIDDLE_CHUNK
    )
    delta = delta[:, :heads].T
    table = jnp.concatenate([lse.reshape(heads, rows), delta], axis=0)
    spread = lambda grad, lead=(): grad.reshape(lead + dims + (2, grad.shape[len(lead)] // devices, grad.shape[-1]))
    (up_owned, down_owned, out_owned), (grad_window, table_window) = scatter(
        [spread(grad_up), spread(grad_down), spread(grad_out)], [grad_mixed, table], devices, EXCHANGE_ORDERS, 1
    )
    grad_window = grad_window.reshape(-1, width)
    table_window = table_window.transpose(1, 0, 2).reshape(2 * heads, -1)
    groups = heads // (2 * GROUP)
    lse_window = table_window[:heads].reshape(groups, 2 * GROUP, -1)
    delta_window = table_window[heads:].reshape(groups, 2 * GROUP, -1)
    grad_query = query_grad(query_window, grad_mixed, key_window, value_window, lse, delta.reshape(lse.shape), lower, upper, query_bounds, rq, rk, GROUP)
    grad_keys, grad_values = key_grad(
        key_window, value_window, query_window, grad_window, lse_window, delta_window,
        starts[None, :], ends[None, :], key_bounds, base, rows, sk, sq, GROUP,
    )
    grad_tokens, grad_qkv, last_rows = last_block(
        tokens, grad_middle, grad_query, grad_keys, grad_values, vector_full, qkv_full, LAST_TILE
    )
    grad_vectors = jnp.concatenate([last_rows[:4], middle_rows[:4], bias_row.reshape(-1, width)], axis=0)
    vector_rows = grad_vectors.reshape(vectors.shape[0], devices, -1).transpose(1, 0, 2).reshape(devices, -1)
    vector_rows = jnp.pad(vector_rows, ((0, 0), (0, 8 * LANE - vector_rows.shape[1]))).reshape(dims + (2, 8, LANE))
    (qkv_owned, vector_owned), _ = scatter([spread(grad_qkv, (3,)), vector_rows], [], devices, SCATTER_ORDERS, 2)
    vector_owned = vector_owned.reshape(-1)[: vectors.size].reshape(vectors.shape)
    owned = (qkv_owned, out_owned, up_owned, down_owned, vector_owned)
    firsts = (qkv_first, out_first, up_first, down_first, vector_first)
    seconds = (qkv_second, out_second, up_second, down_second, vector_second)
    stepped = [adamw_step(*four) for four in zip(shards, owned, firsts, seconds)]
    return (result, grad_tokens) + tuple(stepped[place][kind] for kind in range(3) for place in range(5))


def solution(mesh):
    in_specs = (
        P("dev", None),
        P("dev", None),
        P("dev"),
        P("dev"),
        P(None, "dev", None),
        P("dev", None),
        P("dev", None),
        P("dev", None),
        P(None, "dev"),
        P(None, "dev", None),
        P("dev", None),
        P("dev", None),
        P("dev", None),
        P(None, "dev"),
        P(None, "dev", None),
        P("dev", None),
        P("dev", None),
        P("dev", None),
        P(None, "dev"),
    )
    out_specs = (
        P("dev", None),
        P("dev", None),
        P(None, "dev", None),
        P("dev", None),
        P("dev", None),
        P("dev", None),
        P(None, "dev"),
        P(None, "dev", None),
        P("dev", None),
        P("dev", None),
        P("dev", None),
        P(None, "dev"),
        P(None, "dev", None),
        P("dev", None),
        P("dev", None),
        P("dev", None),
        P(None, "dev"),
    )
    return jax.shard_map(
        per_device, mesh=mesh, in_specs=in_specs, out_specs=out_specs, check_vma=False
    )
```
